32 devices in a mesh: dp: 16 (over z, y, core), tp: 2 (over x).
Axes of the slice: x: 2, y: 2, z: 4, core: 2. Of those that a mesh axis runs over, the one named last changes fastest.
Arguments:
- hidden: bfloat16 [4096, 4096], P(('dp', 'tp')), may hold values from -6 to 6
- query_grad: bfloat16 [4096, 1024], P('dp', 'tp'), may hold values from -1.5 to 1.5
- key_grad: bfloat16 [4096, 256], P('dp', 'tp'), may hold values from -1.5 to 1.5
- value_grad: bfloat16 [4096, 256], P('dp', 'tp'), may hold values from -1.5 to 1.5
- w_query: bfloat16 [4096, 1024], P(None, 'tp'), may hold values from -0.09375 to 0.09375
- w_key: bfloat16 [4096, 256], P(None, 'tp'), may hold values from -0.09375 to 0.09375
- w_value: bfloat16 [4096, 256], P(None, 'tp'), may hold values from -0.09375 to 0.09375
Outputs:
- hidden_grad: bfloat16 [4096, 4096], P(('dp', 'tp'))
- grad_query: float32 [4096, 1024], P('dp', 'tp')
- grad_key: float32 [4096, 256], P('dp', 'tp')
- grad_value: float32 [4096, 256], P('dp', 'tp')
The draws below stay inside these ranges and needn't reach their ends.
All inputs are finite; a program needn't handle non-finite values.
Results may differ from the reference program's by a relative error of at most 0.014.
Values may be sent and summed in bfloat16 or wider, within the bound.
A program may use at most 256 MiB of HBM per device.

```python
import jax
import jax.numpy as jnp
from jax import lax

D = 4096
HEAD = 128
Q_DEV = 4
KV_HEADS = 2
Q_W = 1024
KV_W = 256
GROUP_TOK = 256
TOKENS = 4096
N_DP = 16


def raised(entries, key, source, target, blocks, factor):
    owner, partner = [(jnp.arange(entries.shape[position]) // (entries.shape[position] // blocks)).reshape([-1 if axis == position else 1 for axis in range(entries.ndim)]) for position in (source, target)]
    chosen = jax.random.permutation(key, blocks)[partner]
    strong = (owner == chosen) | (owner == (partner + blocks // 2) % blocks)
    return jnp.where(strong, factor * entries, entries)


def steps_of(stream_key, shape, shards, low, largest):
    gain, own = 1.0, jax.random.fold_in(stream_key, 6)
    for dim, blocks in shards:
        draws = jnp.exp(jax.random.uniform(jax.random.fold_in(own, dim), (blocks,), jnp.float32, low / len(shards), largest / len(shards)))
        gain = gain * jnp.repeat(draws, shape[dim] // blocks).reshape([-1 if axis == dim else 1 for axis in range(len(shape))])
    return gain


def gaussian(key, dims, scale, most, pieces=(), dtype=jnp.bfloat16):
    result = scale * jax.random.normal(key, dims, jnp.float32)
    if pieces:
        result = result * steps_of(key, dims, pieces, -0.22, 0.18)
    return jnp.clip(result, -most, most).astype(dtype)


def noise_with(stream_key, extent, scale, most, split, heavy, kind=jnp.bfloat16):
    array = scale * jax.random.normal(stream_key, extent, jnp.float32)
    if split:
        array = array * steps_of(stream_key, extent, split, -0.22, 0.18)
    return jnp.clip(raised(array, jax.random.fold_in(stream_key, 3), *heavy), -most, most).astype(kind)


def setup_inputs(seed: int = 0) -> dict:
    key_of = jax.random.split(jax.random.key(seed), 8)
    return {
        "hidden": noise_with(key_of[0], (TOKENS, D), 1.0, 6.0, ((0, 32),), (0, 1, 32, 2.75)),
        "query_grad": gaussian(key_of[1], (TOKENS, Q_W), 0.25, 1.5, ((0, 16), (1, 2))),
        "key_grad": gaussian(key_of[2], (TOKENS, KV_W), 0.25, 1.5, ((0, 16), (1, 2))),
        "value_grad": gaussian(key_of[3], (TOKENS, KV_W), 0.25, 1.5, ((0, 16), (1, 2))),
        "w_query": gaussian(key_of[4], (D, Q_W), D ** -0.5, 0.09375, ((1, 2),)),
        "w_key": gaussian(key_of[5], (D, KV_W), D ** -0.5, 0.09375, ((1, 2),)),
        "w_value": gaussian(key_of[6], (D, KV_W), D ** -0.5, 0.09375, ((1, 2),)),
    }


def contract_rows(left, right):
    return lax.dot_general(left, right, (((0,), (0,)), ((), ())), preferred_element_type=jnp.float32)


def rounded(value):
    return lax.optimization_barrier(value.astype(jnp.bfloat16)).astype(jnp.float32)


def reference(hidden, query_grad, key_grad, value_grad, w_query, w_key, w_value):
    hidden_groups = hidden.reshape(N_DP, GROUP_TOK, D)
    query_groups = query_grad.reshape(N_DP, GROUP_TOK, Q_W)
    key_groups = key_grad.reshape(N_DP, GROUP_TOK, KV_W)
    value_groups = value_grad.reshape(N_DP, GROUP_TOK, KV_W)
    weight_heads = jnp.concatenate((w_query.reshape(D, KV_HEADS, Q_DEV * HEAD), w_key.reshape(D, KV_HEADS, HEAD), w_value.reshape(D, KV_HEADS, HEAD)), axis=2).astype(jnp.float32)

    def one_group(totals, inputs):
        grad_wq, grad_wk, grad_wv = totals
        hid, qgr, kgr, vgr = inputs
        grad_heads = jnp.concatenate((qgr.reshape(GROUP_TOK, KV_HEADS, Q_DEV * HEAD), kgr.reshape(GROUP_TOK, KV_HEADS, HEAD), vgr.reshape(GROUP_TOK, KV_HEADS, HEAD)), axis=2).astype(jnp.float32)
        parts = jnp.einsum("thc,dhc->htd", grad_heads, weight_heads)
        hid_grad = jnp.sum(rounded(parts), axis=0).astype(jnp.bfloat16)
        grad_wq = grad_wq + rounded(contract_rows(hid, qgr))
        grad_wk = grad_wk + rounded(contract_rows(hid, kgr))
        grad_wv = grad_wv + rounded(contract_rows(hid, vgr))
        return (grad_wq, grad_wk, grad_wv), hid_grad

    zeros = (jnp.zeros((D, Q_W), jnp.float32), jnp.zeros((D, KV_W), jnp.float32), jnp.zeros((D, KV_W), jnp.float32))
    totals, outputs = lax.scan(one_group, zeros, (hidden_groups, query_groups, key_groups, value_groups))
    hidden_grad = outputs.reshape(TOKENS, D)
    return hidden_grad, totals[0], totals[1], totals[2]
```

```python
import functools

import jax
import jax.numpy as jnp
from jax import lax
from jax.experimental import pallas as pl
from jax.experimental.pallas import tpu as pltpu
from jax.sharding import PartitionSpec as P

MESH = pl.DeviceIdType.MESH


def contract_rows(left, right):
    return lax.dot_general(
        left, right, (((0,), (0,)), ((), ())), preferred_element_type=jnp.float32
    )


def contract_cols(left, right):
    return lax.dot_general(
        left, right, (((1,), (1,)), ((), ())), preferred_element_type=jnp.float32
    )


def local(hidden, query_grad, key_grad, value_grad, w_query, w_key, w_value):
    query_width = w_query.shape[1]
    head_width = w_key.shape[1]
    all_grads = jnp.concatenate((query_grad, key_grad, value_grad), axis=1)
    all_weights = jnp.concatenate((w_query, w_key, w_value), axis=1)
    total = contract_rows(lax.all_gather(hidden, "tp", axis=0, tiled=True), all_grads)
    summed = lax.psum_scatter(
        contract_cols(all_grads, all_weights).astype(jnp.bfloat16),
        "tp",
        scatter_dimension=0,
        tiled=True,
    )
    weight_grad = lax.psum_scatter(
        total.astype(jnp.bfloat16), "dp", scatter_dimension=0, tiled=True
    ).astype(jnp.float32)
    grad_query = weight_grad[:, :query_width]
    grad_key = weight_grad[:, query_width : query_width + head_width]
    grad_value = weight_grad[:, query_width + head_width :]
    return (summed, grad_query, grad_key, grad_value)


def targets(n_z, z):
    near_low = z < n_z - 1 - z
    return sorted(
        range(n_z), key=lambda t: (-abs(t - z), t if near_low else -t)
    )


def pick(values, index):
    chosen = jnp.int32(values[0])
    for i, value in enumerate(values[1:]):
        chosen = jnp.where(index == i + 1, jnp.int32(value), chosen)
    return chosen


def kernel(
    n_z, pieces, n_c,
    hidden, query_grad, key_grad, value_grad, w_query, w_key, w_value,
    result, final,
    tokens, grads, weights, head_out, head_in, core_out, core_in,
    total, z_out, z_in, own_head,
    load_sem, own_send, own_recv, fwd_send, fwd_recv, ytok_send, ytok_recv,
    ygrad_send, ygrad_recv, head_send, head_recv, core_send, core_recv,
    z_send, z_recv,
):
    dp = lax.axis_index("dp")
    tp = lax.axis_index("tp")
    core = lax.rem(dp, 2)
    y = lax.rem(dp // 2, 2)
    z = dp // 4
    half = hidden.shape[0]
    group = query_grad.shape[0]
    q_w = query_grad.shape[1]
    k_w = key_grad.shape[1]
    rows = final.shape[0]
    pair = 2 * rows
    width = hidden.shape[1] // pieces
    chunk = 2 * k_w
    bf16, f32 = jnp.bfloat16, jnp.float32

    x_peer = (dp, 1 - tp)
    core_peer = (dp + 1 - 2 * core, tp)
    y_peer = (dp + 2 - 4 * y, tp)
    at_low, at_high = z == 0, z == n_z - 1
    at_end = jnp.logical_or(at_low, at_high)

    order = [targets(n_z, i) for i in range(n_z)]
    target = [pick([order[i][k] for i in range(n_z)], z) for k in range(n_z)]
    down = [jnp.where(target[k] < z, 1, 0) for k in range(n_z)]

    mine = pl.ds(pl.multiple_of(tp * half, half), half)
    theirs = pl.ds(pl.multiple_of((1 - tp) * half, half), half)
    mine_far = pl.ds(pl.multiple_of(group + tp * half, half), half)

    def columns_of(k, side):
        return pl.ds(pl.multiple_of((target[k] * 2 + side) * pair, pair), pair)

    def load(index, source, place):
        copy = pltpu.make_async_copy(source, place, load_sem.at[index])
        copy.start()
        return copy

    near = pl.ds(0, group)
    far = pl.ds(group, group)
    grad_loads = [
        load(0, query_grad, grads.at[near, pl.ds(0, q_w)]),
        load(1, key_grad, grads.at[near, pl.ds(q_w, k_w)]),
        load(2, value_grad, grads.at[near, pl.ds(q_w + k_w, k_w)]),
    ]
    weight_loads = [
        load(3, w_query, weights.at[:, pl.ds(0, q_w)]),
        load(4, w_key, weights.at[:, pl.ds(q_w, k_w)]),
        load(5, w_value, weights.at[:, pl.ds(q_w + k_w, k_w)]),
    ]
    token_loads = [
        load(6 + k, hidden.at[:, columns_of(k, y)], tokens.at[k, mine, :])
        for k in range(n_z)
    ]

    barrier = pltpu.get_barrier_semaphore()

    def greet(peer):
        pl.semaphore_signal(barrier, inc=1, device_id=peer, device_id_type=MESH)

    for peer in (x_peer, y_peer, core_peer):
        greet(peer)

    @pl.when(jnp.logical_not(at_low))
    def _():
        greet((dp - 4, tp))

    @pl.when(jnp.logical_not(at_high))
    def _():
        greet((dp + 4, tp))

    pl.semaphore_wait(barrier, 5 - jnp.where(at_end, 1, 0))

    def remote(source, place, send, recv, peer):
        return pltpu.make_async_remote_copy(
            src_ref=source, dst_ref=place, send_sem=send, recv_sem=recv,
            device_id=peer, device_id_type=MESH,
        )

    own_copies = [
        remote(
            hidden.at[:, columns_of(k, y)], tokens.at[k, mine, :],
            own_send.at[k], own_recv.at[k], x_peer,
        )
        for k in range(n_z)
    ]
    fwd_copies = [
        remote(
            tokens.at[k, mine_far, :], tokens.at[k, mine_far, :],
            fwd_send.at[k], fwd_recv.at[k], x_peer,
        )
        for k in range(n_z)
    ]
    ytok_copies = [
        remote(
            hidden.at[:, columns_of(k, 1 - y)], tokens.at[k, mine_far, :],
            ytok_send.at[k], ytok_recv.at[k], y_peer,
        )
        for k in range(n_z)
    ]
    ygrad_copies = [
        [
            remote(
                query_grad.at[:, pl.ds(n * chunk, chunk)],
                grads.at[far, pl.ds(n * chunk, chunk)],
                ygrad_send.at[n], ygrad_recv.at[n], y_peer,
            )
        ]
        for n in range(n_c - 1)
    ] + [
        [
            remote(
                source, grads.at[far, pl.ds(q_w + i * k_w, k_w)],
                ygrad_send.at[n_c - 1 + i], ygrad_recv.at[n_c - 1 + i], y_peer,
            )
            for i, source in enumerate((key_grad, value_grad))
        ]
    ]
    head_copies = [
        remote(
            head_out.at[j], head_in.at[j], head_send.at[j], head_recv.at[j], x_peer
        )
        for j in range(pieces)
    ]
    core_copies = [
        [
            remote(
                core_out.at[k, n], core_in.at[k, n],
                core_send.at[k, n], core_recv.at[k, n], core_peer,
            )
            for n in range(n_c)
        ]
        for k in range(n_z)
    ]
    z_copies = [
        [
            remote(
                z_out.at[k, n], z_in.at[down[k], target[k], n],
                z_send.at[k, n], z_recv.at[down[k], target[k], n],
                (dp + 4 - 8 * down[k], tp),
            )
            for n in range(n_c)
        ]
        for k in range(n_z - 1)
    ]

    own_copies[0].start()
    ytok_copies[0].start()
    own_copies[1].start()
    for n in range(n_c - 1):
        ygrad_copies[n][0].start()
    ytok_copies[1].start()
    for copy in ygrad_copies[n_c - 1]:
        copy.start()
    for copy in ytok_copies[2:]:
        copy.start()

    for copy in grad_loads + weight_loads:
        copy.wait()

    def head_piece(j):
        columns = pl.ds(j * width, width)
        head_out[j] = contract_cols(grads[theirs, :], weights[columns, :]).astype(bf16)
        own_head[:, columns] = contract_cols(grads[mine, :], weights[columns, :])

    def block(k, n, which):
        start = pl.multiple_of(which * rows, rows)
        return contract_rows(
            tokens[k, :, pl.ds(start, rows)], grads[:, pl.ds(n * chunk, chunk)]
        )

    def arrive(k):
        token_loads[k].wait()
        own_copies[k].wait_recv()
        fwd_copies[k].wait_recv()

    def partial(k, n):
        if k == 0:
            for copy in ygrad_copies[n]:
                copy.wait_recv()
        core_out[k, n] = block(k, n, 1 - core).astype(bf16)
        core_copies[k][n].start()
        total[k, n] = block(k, n, core)

    def pass_on(k, n, at_line_end):
        def run():
            core_copies[k][n].wait_recv()
            summed = total[k, n] + core_in[k, n].astype(f32)
            if not at_line_end:
                z_copies[k][n].wait_recv()
                summed = summed + z_in[down[k], target[k], n].astype(f32)
            z_out[k, n] = summed.astype(bf16)
            z_copies[k][n].start()

        pl.when(at_end if at_line_end else jnp.logical_not(at_end))(run)

    def from_line(direction, n):
        return remote(
            z_out.at[0, n], z_in.at[direction, z, n],
            z_send.at[0, n], z_recv.at[direction, z, n], x_peer,
        )

    def finish(n):
        last = n_z - 1
        span = pl.ds(n * chunk, chunk)
        core_copies[last][n].wait_recv()
        final[:, span] = total[last, n] + core_in[last, n].astype(f32)

        for direction, edge in ((0, at_low), (1, at_high)):
            @pl.when(jnp.logical_not(edge))
            def _():
                from_line(direction, n).wait_recv()
                final[:, span] += z_in[direction, z, n].astype(f32)

    def add_heads(j):
        head_copies[j].wait_recv()
        columns = pl.ds(j * width, width)
        own = own_head[:, columns]
        result[:, columns] = (own + head_in[j].astype(f32)).astype(result.dtype)

    chunks = range(n_c)
    ready = sent = 0

    def prepare(count):
        nonlocal ready
        for j in range(ready, min(ready + count, pieces)):
            head_piece(j)
        ready = min(ready + count, pieces)

    def send_heads(count):
        nonlocal sent
        for j in range(sent, min(sent + count, ready)):
            head_copies[j].start()
        sent = min(sent + count, ready)

    prepare(3)
    ytok_copies[0].wait_recv()
    fwd_copies[0].start()
    for copy in own_copies[2:]:
        copy.start()
    prepare(2)
    arrive(0)
    for n in chunks[:-1]:
        partial(0, n)
    for n in chunks[:-1]:
        pass_on(0, n, True)
    for k in range(1, n_z):
        ytok_copies[k].wait_recv()
        fwd_copies[k].start()
        send_heads(1 if k < n_z - 1 else pieces)
        if k == 1:
            partial(0, n_c - 1)
            pass_on(0, n_c - 1, True)
        prepare(1 if k < n_z - 1 else pieces)
        send_heads(0 if k < n_z - 1 else pieces)
        if k >= 2:
            arrive(k - 1)
            for n in chunks:
                partial(k - 1, n)
                if n > 0:
                    pass_on(k - 1, n - 1, True)
            pass_on(k - 1, n_c - 1, True)
            for n in chunks:
                pass_on(k - 2, n, False)
    arrive(n_z - 1)
    for n in chunks:
        partial(n_z - 1, n)
    for n in chunks:
        pass_on(n_z - 2, n, False)
    for n in chunks:
        finish(n)
    for j in range(pieces):
        add_heads(j)
    grad_sends = [copy for copies in ygrad_copies for copy in copies]
    flat = [copy for copies in core_copies + z_copies for copy in copies]
    for copy in own_copies + fwd_copies + ytok_copies + grad_sends + head_copies + flat:
        copy.wait_send()


def place(result, final, out_hidden, out_query, out_key, out_value, sem):
    q_w, k_w = out_query.shape[1], out_key.shape[1]
    copies = [
        pltpu.make_async_copy(result, out_hidden, sem.at[0]),
        pltpu.make_async_copy(final.at[:, pl.ds(0, q_w)], out_query, sem.at[1]),
        pltpu.make_async_copy(final.at[:, pl.ds(q_w, k_w)], out_key, sem.at[2]),
        pltpu.make_async_copy(
            final.at[:, pl.ds(q_w + k_w, k_w)], out_value, sem.at[3]
        ),
    ]
    for copy in copies:
        copy.start()
    for copy in copies:
        copy.wait()


def fused(n_dp, hidden, query_grad, key_grad, value_grad, w_query, w_key, w_value):
    half, depth = hidden.shape
    group = query_grad.shape[0]
    q_w, k_w = w_query.shape[1], w_key.shape[1]
    wide = q_w + 2 * k_w
    rows = depth // n_dp
    if q_w % (2 * k_w) or rows % 128 or k_w % 128 or half * 2 != group:
        return local(hidden, query_grad, key_grad, value_grad, w_query, w_key, w_value)
    n_z = n_dp // 4
    n_c = wide // (2 * k_w)
    chunk = 2 * k_w
    pieces = 2 * n_z
    width = depth // pieces
    bf16, f32 = jnp.bfloat16, jnp.float32
    dma = pltpu.SemaphoreType.DMA
    held = pl.pallas_call(
        functools.partial(kernel, n_z, pieces, n_c),
        out_shape=(pltpu.VMEM((half, depth), bf16), pltpu.VMEM((rows, wide), f32)),
        in_specs=[pl.BlockSpec(memory_space=pl.ANY)] * 7,
        out_specs=(pl.BlockSpec(memory_space=pltpu.VMEM),) * 2,
        scratch_shapes=[
            pltpu.VMEM((n_z, 2 * group, 2 * rows), bf16),
            pltpu.VMEM((2 * group, wide), bf16),
            pltpu.VMEM((depth, wide), bf16),
            pltpu.VMEM((pieces, half, width), bf16),
            pltpu.VMEM((pieces, half, width), bf16),
            pltpu.VMEM((n_z, n_c, rows, chunk), bf16),
            pltpu.VMEM((n_z, n_c, rows, chunk), bf16),
            pltpu.VMEM((n_z, n_c, rows, chunk), f32),
            pltpu.VMEM((n_z - 1, n_c, rows, chunk), bf16),
            pltpu.VMEM((2, n_z, n_c, rows, chunk), bf16),
            pltpu.VMEM((half, depth), f32),
            dma((6 + n_z,)),
            dma((n_z,)), dma((n_z,)),
            dma((n_z,)), dma((n_z,)),
            dma((n_z,)), dma((n_z,)),
            dma((n_c + 1,)), dma((n_c + 1,)),
            dma((pieces,)), dma((pieces,)),
            dma((n_z, n_c)), dma((n_z, n_c)),
            dma((n_z - 1, n_c)), dma((2, n_z, n_c)),
        ],
        compiler_params=pltpu.CompilerParams(
            collective_id=0, has_side_effects=True, vmem_limit_bytes=56 * 1024 * 1024
        ),
    )(hidden, query_grad, key_grad, value_grad, w_query, w_key, w_value)
    return pl.pallas_call(
        place,
        out_shape=(
            jax.ShapeDtypeStruct((half, depth), bf16),
            jax.ShapeDtypeStruct((rows, q_w), f32),
            jax.ShapeDtypeStruct((rows, k_w), f32),
            jax.ShapeDtypeStruct((rows, k_w), f32),
        ),
        in_specs=[pl.BlockSpec(memory_space=pltpu.VMEM)] * 2,
        out_specs=(pl.BlockSpec(memory_space=pl.ANY),) * 4,
        scratch_shapes=[dma((4,))],
    )(*[pltpu.with_memory_space_constraint(a, pltpu.VMEM) for a in held])


def solution(mesh):
    placed = (
        P(("dp", "tp"), None),
        P("dp", "tp"),
        P("dp", "tp"),
        P("dp", "tp"),
        P(None, "tp"),
        P(None, "tp"),
        P(None, "tp"),
    )
    n_dp, n_tp = mesh.shape["dp"], mesh.shape["tp"]
    body = local
    if n_tp == 2 and n_dp % 4 == 0 and n_dp > 8:
        body = functools.partial(fused, n_dp)
    return jax.shard_map(
        body,
        mesh=mesh,
        in_specs=placed,
        out_specs=(P(("dp", "tp"), None), P("dp", "tp"), P("dp", "tp"), P("dp", "tp")),
        check_vma=False,
    )
```

```python
import functools

import jax
import jax.numpy as jnp
from jax import lax
from jax.experimental import pallas as pl
from jax.experimental.pallas import tpu as pltpu
from jax.sharding import PartitionSpec as P

MESH = pl.DeviceIdType.MESH


def contract_rows(left, right):
    return lax.dot_general(
        left, right, (((0,), (0,)), ((), ())), preferred_element_type=jnp.float32
    )


def contract_cols(left, right):
    return lax.dot_general(
        left, right, (((1,), (1,)), ((), ())), preferred_element_type=jnp.float32
    )


def local(hidden, query_grad, key_grad, value_grad, w_query, w_key, w_value):
    query_width = w_query.shape[1]
    head_width = w_key.shape[1]
    all_grads = jnp.concatenate((query_grad, key_grad, value_grad), axis=1)
    all_weights = jnp.concatenate((w_query, w_key, w_value), axis=1)
    total = contract_rows(lax.all_gather(hidden, "tp", axis=0, tiled=True), all_grads)
    summed = lax.psum_scatter(
        contract_cols(all_grads, all_weights).astype(jnp.bfloat16),
        "tp",
        scatter_dimension=0,
        tiled=True,
    )
    weight_grad = lax.psum_scatter(
        total.astype(jnp.bfloat16), "dp", scatter_dimension=0, tiled=True
    ).astype(jnp.float32)
    grad_query = weight_grad[:, :query_width]
    grad_key = weight_grad[:, query_width : query_width + head_width]
    grad_value = weight_grad[:, query_width + head_width :]
    return (summed, grad_query, grad_key, grad_value)


def targets(n_z, z):
    near_low = z < n_z - 1 - z
    return sorted(
        range(n_z), key=lambda t: (-abs(t - z), t if near_low else -t)
    )


def pick(values, index):
    chosen = jnp.int32(values[0])
    for i, value in enumerate(values[1:]):
        chosen = jnp.where(index == i + 1, jnp.int32(value), chosen)
    return chosen


def kernel(
    n_z, pieces, n_c,
    hidden, query_grad, key_grad, value_grad, w_query, w_key, w_value,
    result, final,
    tokens, grads, weights, head_out, head_in, core_out, core_in,
    total, z_out, z_in, own_head,
    load_sem, send_sem, x_recv, ytok_recv, ygrad_recv, head_recv, core_recv, z_recv,
    seen_sem, go_sem,
):
    dp = lax.axis_index("dp")
    tp = lax.axis_index("tp")
    core = lax.rem(dp, 2)
    y = lax.rem(dp // 2, 2)
    z = dp // 4
    half = hidden.shape[0]
    group = query_grad.shape[0]
    q_w = query_grad.shape[1]
    k_w = key_grad.shape[1]
    rows = final.shape[0]
    pair = 2 * rows
    width = hidden.shape[1] // pieces
    chunk = 2 * k_w
    bf16, f32 = jnp.bfloat16, jnp.float32

    x_peer = (dp, 1 - tp)
    core_peer = (dp + 1 - 2 * core, tp)
    y_peer = (dp + 2 - 4 * y, tp)
    at_low, at_high = z == 0, z == n_z - 1
    at_end = jnp.logical_or(at_low, at_high)

    order = [targets(n_z, i) for i in range(n_z)]
    target = [pick([order[i][k] for i in range(n_z)], z) for k in range(n_z)]
    down = [jnp.where(target[k] < z, 1, 0) for k in range(n_z)]

    mine = pl.ds(pl.multiple_of(tp * half, half), half)
    theirs = pl.ds(pl.multiple_of((1 - tp) * half, half), half)
    mine_far = pl.ds(pl.multiple_of(group + tp * half, half), half)

    def columns_of(k, side):
        return pl.ds(pl.multiple_of((target[k] * 2 + side) * pair, pair), pair)

    def load(index, source, place):
        pltpu.make_async_copy(source, place, load_sem.at[index]).start()

    near = pl.ds(0, group)
    far = pl.ds(group, group)
    load(0, query_grad, grads.at[near, pl.ds(0, q_w)])
    load(0, key_grad, grads.at[near, pl.ds(q_w, k_w)])
    load(0, value_grad, grads.at[near, pl.ds(q_w + k_w, k_w)])
    load(1, w_query, weights.at[:, pl.ds(0, q_w)])
    load(1, w_key, weights.at[:, pl.ds(q_w, k_w)])
    load(1, w_value, weights.at[:, pl.ds(q_w + k_w, k_w)])
    for k in range(n_z):
        load(2, hidden.at[:, columns_of(k, y)], tokens.at[k, mine, :])

    barrier = pltpu.get_barrier_semaphore()

    def greet(peer):
        pl.semaphore_signal(barrier, inc=1, device_id=peer, device_id_type=MESH)

    greet(x_peer)
    greet(core_peer)
    scout = core == 0
    low_peer, high_peer = (dp - 4, tp), (dp + 4, tp)
    around = 3 - jnp.where(at_end, 1, 0)

    def around_line(tell):
        tell(y_peer)
        pl.when(jnp.logical_not(at_low))(lambda: tell(low_peer))
        pl.when(jnp.logical_not(at_high))(lambda: tell(high_peer))

    pl.when(scout)(lambda: around_line(greet))
    pl.semaphore_wait(barrier, 2 + jnp.where(scout, around, 0))

    def notify(semaphore, peer):
        pl.semaphore_signal(semaphore, inc=1, device_id=peer, device_id_type=MESH)

    def remote(source, place, send, recv, peer):
        return pltpu.make_async_remote_copy(
            src_ref=source, dst_ref=place, send_sem=send, recv_sem=recv,
            device_id=peer, device_id_type=MESH,
        )

    own_copies = [
        remote(
            hidden.at[:, columns_of(k, y)], tokens.at[k, mine, :],
            send_sem.at[0], x_recv.at[k], x_peer,
        )
        for k in range(n_z)
    ]
    fwd_copies = [
        remote(
            tokens.at[k, mine_far, :], tokens.at[k, mine_far, :],
            send_sem.at[1], x_recv.at[k], x_peer,
        )
        for k in range(n_z)
    ]
    ytok_copies = [
        remote(
            hidden.at[:, columns_of(k, 1 - y)], tokens.at[k, mine_far, :],
            send_sem.at[2], ytok_recv.at[k], y_peer,
        )
        for k in range(n_z)
    ]

    def ygrad(source, first, n):
        span = pl.ds(first, source.shape[1])
        return remote(
            source, grads.at[far, span], send_sem.at[3], ygrad_recv.at[n], y_peer
        )

    ygrad_copies = [
        [ygrad(query_grad.at[:, pl.ds(n * chunk, chunk)], n * chunk, n)]
        for n in range(n_c - 1)
    ] + [[ygrad(key_grad, q_w, n_c - 1), ygrad(value_grad, q_w + k_w, n_c - 1)]]
    head_copies = [
        remote(
            head_out.at[j], head_in.at[j], send_sem.at[4], head_recv.at[j], x_peer
        )
        for j in range(pieces)
    ]
    core_copies = [
        [
            remote(
                core_out.at[k, n], core_in.at[k, n],
                send_sem.at[5], core_recv.at[n if k == 0 else n_c + k - 1], core_peer,
            )
            for n in range(n_c)
        ]
        for k in range(n_z)
    ]
    def place_on(step, below):
        i = below + 1 if order[below][step] > below else below - 1
        if not 0 <= i < n_z or order[below][step] == below:
            return 0
        to = order[below][step]
        if to == i:
            return n_z - 1 if below < i else n_z
        return order[i].index(to)

    z_slot = [pick([place_on(k, i) for i in range(n_z)], z) for k in range(n_z - 1)]
    z_copies = [
        [
            remote(
                z_out.at[k, n], z_in.at[z_slot[k], n],
                send_sem.at[6], z_recv.at[z_slot[k], n],
                (dp + 4 - 8 * down[k], tp),
            )
            for n in range(n_c)
        ]
        for k in range(n_z - 1)
    ]

    def landed(whole, semaphore):
        pltpu.make_async_copy(whole, whole, semaphore).wait()

    for copy in own_copies[:3]:
        copy.start()

    def start_y():
        ytok_copies[0].start()
        for n in range(n_c - 1):
            ygrad_copies[n][0].start()
        ytok_copies[1].start()
        for copy in ygrad_copies[n_c - 1]:
            copy.start()
        for copy in ytok_copies[2:]:
            copy.start()

    @pl.when(scout)
    def _():
        start_y()
        around_line(lambda peer: notify(seen_sem, peer))
        pl.semaphore_wait(seen_sem, around)
        notify(go_sem, core_peer)

    @pl.when(jnp.logical_not(scout))
    def _():
        pl.semaphore_wait(go_sem, 1)
        start_y()

    def loaded(index, whole):
        pltpu.make_async_copy(whole, whole, load_sem.at[index]).wait()

    loaded(0, grads.at[near, :])
    loaded(1, weights)

    def head_piece(j):
        columns = pl.ds(j * width, width)
        head_out[j] = contract_cols(grads[theirs, :], weights[columns, :]).astype(bf16)
        own_head[:, columns] = contract_cols(grads[mine, :], weights[columns, :])

    def block(k, n, which):
        start = pl.multiple_of(which * rows, rows)
        return contract_rows(
            tokens[k, :, pl.ds(start, rows)], grads[:, pl.ds(n * chunk, chunk)]
        )

    def arrive(k):
        if k == 0:
            loaded(2, tokens.at[:, mine, :])
        landed(tokens.at[k, pl.ds(0, group), :], x_recv.at[k])

    def partial(k, n):
        if k == 0:
            landed(grads.at[far, pl.ds(n * chunk, chunk)], ygrad_recv.at[n])
        core_out[k, n] = block(k, n, 1 - core).astype(bf16)
        core_copies[k][n].start()
        total[k, n] = block(k, n, core)

    def sibling_part(k, n):
        if k == 0:
            landed(core_in.at[k, n], core_recv.at[n])
        elif n == 0:
            landed(core_in.at[k], core_recv.at[n_c + k - 1])
        return core_in[k, n].astype(f32)

    def pass_on(k, n, at_line_end):
        def run():
            summed = total[k, n] + sibling_part(k, n)
            if not at_line_end:
                landed(z_in.at[k, n], z_recv.at[k, n])
                summed = summed + z_in[k, n].astype(f32)
            z_out[k, n] = summed.astype(bf16)
            z_copies[k][n].start()

        pl.when(at_end if at_line_end else jnp.logical_not(at_end))(run)

    def finish(n):
        last = n_z - 1
        span = pl.ds(n * chunk, chunk)
        final[:, span] = total[last, n] + sibling_part(last, n)

        for slot, edge in ((n_z - 1, at_low), (n_z, at_high)):
            @pl.when(jnp.logical_not(edge))
            def _():
                landed(z_in.at[slot, n], z_recv.at[slot, n])
                final[:, span] += z_in[slot, n].astype(f32)

    def add_heads(j):
        head_copies[j].wait_recv()
        columns = pl.ds(j * width, width)
        own = own_head[:, columns]
        result[:, columns] = (own + head_in[j].astype(f32)).astype(result.dtype)

    chunks = range(n_c)
    ready = sent = 0

    def prepare(count):
        nonlocal ready
        for j in range(ready, min(ready + count, pieces)):
            head_piece(j)
        ready = min(ready + count, pieces)

    def send_heads(count):
        nonlocal sent
        for j in range(sent, min(sent + count, ready)):
            head_copies[j].start()
        sent = min(sent + count, ready)

    prepare(3)
    ytok_copies[0].wait_recv()
    fwd_copies[0].start()
    for copy in own_copies[3:]:
        copy.start()
    send_heads(1)
    prepare(2)
    arrive(0)
    for n in chunks[:-1]:
        partial(0, n)
    for n in chunks[:-1]:
        pass_on(0, n, True)
    for k in range(1, n_z):
        ytok_copies[k].wait_recv()
        fwd_copies[k].start()
        send_heads(1 if k < n_z - 1 else pieces)
        if k == 1:
            partial(0, n_c - 1)
            pass_on(0, n_c - 1, True)
        prepare(1 if k < n_z - 1 else pieces)
        send_heads(0 if k < n_z - 1 else pieces)
        if k >= 2:
            arrive(k - 1)
            for n in chunks:
                partial(k - 1, n)
            for n in chunks:
                pass_on(k - 1, n, True)
            for n in chunks:
                pass_on(k - 2, n, False)
    arrive(n_z - 1)
    for n in chunks:
        partial(n_z - 1, n)
    for n in chunks:
        pass_on(n_z - 2, n, False)
    for n in chunks:
        finish(n)
    for j in range(pieces):
        add_heads(j)
    sources = (
        tokens.at[:, mine, :], tokens.at[:, mine, :], tokens.at[:, mine, :],
        grads.at[near, :], head_out, core_out, z_out,
    )
    for i, source in enumerate(sources):
        landed(source, send_sem.at[i])


def place(result, final, out_hidden, out_query, out_key, out_value, sem):
    q_w, k_w = out_query.shape[1], out_key.shape[1]
    copies = [
        pltpu.make_async_copy(result, out_hidden, sem.at[0]),
        pltpu.make_async_copy(final.at[:, pl.ds(0, q_w)], out_query, sem.at[1]),
        pltpu.make_async_copy(final.at[:, pl.ds(q_w, k_w)], out_key, sem.at[2]),
        pltpu.make_async_copy(
            final.at[:, pl.ds(q_w + k_w, k_w)], out_value, sem.at[3]
        ),
    ]
    for copy in copies:
        copy.start()
    for copy in copies:
        copy.wait()


def fused(n_dp, hidden, query_grad, key_grad, value_grad, w_query, w_key, w_value):
    half, depth = hidden.shape
    group = query_grad.shape[0]
    q_w, k_w = w_query.shape[1], w_key.shape[1]
    wide = q_w + 2 * k_w
    rows = depth // n_dp
    if q_w % (2 * k_w) or rows % 128 or k_w % 128 or half * 2 != group:
        return local(hidden, query_grad, key_grad, value_grad, w_query, w_key, w_value)
    n_z = n_dp // 4
    n_c = wide // (2 * k_w)
    chunk = 2 * k_w
    pieces = 2 * n_z
    width = depth // pieces
    bf16, f32 = jnp.bfloat16, jnp.float32
    dma = pltpu.SemaphoreType.DMA
    held = pl.pallas_call(
        functools.partial(kernel, n_z, pieces, n_c),
        out_shape=(pltpu.VMEM((half, depth), bf16), pltpu.VMEM((rows, wide), f32)),
        in_specs=[pl.BlockSpec(memory_space=pl.ANY)] * 7,
        out_specs=(pl.BlockSpec(memory_space=pltpu.VMEM),) * 2,
        scratch_shapes=[
            pltpu.VMEM((n_z, 2 * group, 2 * rows), bf16),
            pltpu.VMEM((2 * group, wide), bf16),
            pltpu.VMEM((depth, wide), bf16),
            pltpu.VMEM((pieces, half, width), bf16),
            pltpu.VMEM((pieces, half, width), bf16),
            pltpu.VMEM((n_z, n_c, rows, chunk), bf16),
            pltpu.VMEM((n_z, n_c, rows, chunk), bf16),
            pltpu.VMEM((n_z, n_c, rows, chunk), f32),
            pltpu.VMEM((n_z - 1, n_c, rows, chunk), bf16),
            pltpu.VMEM((n_z + 1, n_c, rows, chunk), bf16),
            pltpu.VMEM((half, depth), f32),
            dma((3,)), dma((7,)), dma((n_z,)), dma((n_z,)), dma((n_c,)), dma((pieces,)),
            dma((n_c + n_z - 1,)), dma((n_z + 1, n_c)),
            pltpu.SemaphoreType.REGULAR, pltpu.SemaphoreType.REGULAR,
        ],
        compiler_params=pltpu.CompilerParams(
            collective_id=0, has_side_effects=True, vmem_limit_bytes=56 * 1024 * 1024
        ),
    )(hidden, query_grad, key_grad, value_grad, w_query, w_key, w_value)
    return pl.pallas_call(
        place,
        out_shape=(
            jax.ShapeDtypeStruct((half, depth), bf16),
            jax.ShapeDtypeStruct((rows, q_w), f32),
            jax.ShapeDtypeStruct((rows, k_w), f32),
            jax.ShapeDtypeStruct((rows, k_w), f32),
        ),
        in_specs=[pl.BlockSpec(memory_space=pltpu.VMEM)] * 2,
        out_specs=(pl.BlockSpec(memory_space=pl.ANY),) * 4,
        scratch_shapes=[dma((4,))],
    )(*[pltpu.with_memory_space_constraint(a, pltpu.VMEM) for a in held])


def solution(mesh):
    placed = (
        P(("dp", "tp"), None),
        P("dp", "tp"),
        P("dp", "tp"),
        P("dp", "tp"),
        P(None, "tp"),
        P(None, "tp"),
        P(None, "tp"),
    )
    n_dp, n_tp = mesh.shape["dp"], mesh.shape["tp"]
    body = local
    if n_tp == 2 and n_dp % 4 == 0 and n_dp > 8:
        body = functools.partial(fused, n_dp)
    return jax.shard_map(
        body,
        mesh=mesh,
        in_specs=placed,
        out_specs=(P(("dp", "tp"), None), P("dp", "tp"), P("dp", "tp"), P("dp", "tp")),
        check_vma=False,
    )
```

```python
import functools

import jax
import jax.numpy as jnp
from jax import lax
from jax.experimental import pallas as pl
from jax.experimental.pallas import tpu as pltpu
from jax.sharding import PartitionSpec as P

MESH = pl.DeviceIdType.MESH


def contract_rows(left, right):
    return lax.dot_general(
        left, right, (((0,), (0,)), ((), ())), preferred_element_type=jnp.float32
    )


def contract_cols(left, right):
    return lax.dot_general(
        left, right, (((1,), (1,)), ((), ())), preferred_element_type=jnp.float32
    )


def local(hidden, query_grad, key_grad, value_grad, w_query, w_key, w_value):
    query_width = w_query.shape[1]
    head_width = w_key.shape[1]
    all_grads = jnp.concatenate((query_grad, key_grad, value_grad), axis=1)
    all_weights = jnp.concatenate((w_query, w_key, w_value), axis=1)
    total = contract_rows(lax.all_gather(hidden, "tp", axis=0, tiled=True), all_grads)
    summed = lax.psum_scatter(
        contract_cols(all_grads, all_weights).astype(jnp.bfloat16),
        "tp",
        scatter_dimension=0,
        tiled=True,
    )
    weight_grad = lax.psum_scatter(
        total.astype(jnp.bfloat16), "dp", scatter_dimension=0, tiled=True
    ).astype(jnp.float32)
    grad_query = weight_grad[:, :query_width]
    grad_key = weight_grad[:, query_width : query_width + head_width]
    grad_value = weight_grad[:, query_width + head_width :]
    return (summed, grad_query, grad_key, grad_value)


def targets(n_z, z):
    near_low = z < n_z - 1 - z
    return sorted(
        range(n_z), key=lambda t: (-abs(t - z), t if near_low else -t)
    )


def pick(values, index):
    chosen = jnp.int32(values[0])
    for i, value in enumerate(values[1:]):
        chosen = jnp.where(index == i + 1, jnp.int32(value), chosen)
    return chosen


def kernel(
    n_z, pieces, n_c,
    hidden, query_grad, key_grad, value_grad, w_query, w_key, w_value,
    result, final,
    tokens, grads, weights, head_out, head_in, core_out, core_in,
    total, z_out, z_in, own_head, gathered, own_grads,
    load_sem, send_sem, x_recv, ytok_recv, ygrad_recv, head_recv, core_recv, z_recv,
    unit_send, unit_recv, plane_recv, seen_sem, go_sem,
):
    dp = lax.axis_index("dp")
    tp = lax.axis_index("tp")
    core = lax.rem(dp, 2)
    y = lax.rem(dp // 2, 2)
    z = dp // 4
    half = hidden.shape[0]
    group = query_grad.shape[0]
    q_w = query_grad.shape[1]
    k_w = key_grad.shape[1]
    rows = final.shape[0]
    pair = 2 * rows
    width = hidden.shape[1] // 2 // pieces
    own_first = hidden.shape[1] // 2
    unit = rows // 2
    chunk = 2 * k_w
    bf16, f32 = jnp.bfloat16, jnp.float32

    x_peer = (dp, 1 - tp)
    core_peer = (dp + 1 - 2 * core, tp)
    y_peer = (dp + 2 - 4 * y, tp)
    at_low, at_high = z == 0, z == n_z - 1
    at_end = jnp.logical_or(at_low, at_high)

    order = [targets(n_z, i) for i in range(n_z)]
    target = [pick([order[i][k] for i in range(n_z)], z) for k in range(n_z)]
    down = [jnp.where(target[k] < z, 1, 0) for k in range(n_z)]

    mine = pl.ds(pl.multiple_of(tp * half, half), half)
    theirs = pl.ds(pl.multiple_of((1 - tp) * half, half), half)
    mine_far = pl.ds(pl.multiple_of(group + tp * half, half), half)

    def columns_of(k, side):
        return pl.ds(pl.multiple_of((target[k] * 2 + side) * pair, pair), pair)

    def load(index, source, place):
        pltpu.make_async_copy(source, place, load_sem.at[index]).start()

    near = pl.ds(0, group)
    far = pl.ds(group, group)
    load(0, query_grad, grads.at[near, pl.ds(0, q_w)])
    load(0, key_grad, grads.at[near, pl.ds(q_w, k_w)])
    load(0, value_grad, grads.at[near, pl.ds(q_w + k_w, k_w)])
    load(1, w_query, weights.at[:, pl.ds(0, q_w)])
    load(1, w_key, weights.at[:, pl.ds(q_w, k_w)])
    load(1, w_value, weights.at[:, pl.ds(q_w + k_w, k_w)])
    for k in range(n_z):
        load(2, hidden.at[:, columns_of(k, y)], tokens.at[k, mine, :])

    barrier = pltpu.get_barrier_semaphore()

    def greet(peer):
        pl.semaphore_signal(barrier, inc=1, device_id=peer, device_id_type=MESH)

    greet(x_peer)
    greet(core_peer)
    scout = core == 0
    low_peer, high_peer = (dp - 4, tp), (dp + 4, tp)
    around = 3 - jnp.where(at_end, 1, 0)

    def around_line(tell):
        tell(y_peer)
        pl.when(jnp.logical_not(at_low))(lambda: tell(low_peer))
        pl.when(jnp.logical_not(at_high))(lambda: tell(high_peer))

    pl.when(scout)(lambda: around_line(greet))
    pl.semaphore_wait(barrier, 2 + jnp.where(scout, around, 0))

    def notify(semaphore, peer):
        pl.semaphore_signal(semaphore, inc=1, device_id=peer, device_id_type=MESH)

    def remote(source, place, send, recv, peer):
        return pltpu.make_async_remote_copy(
            src_ref=source, dst_ref=place, send_sem=send, recv_sem=recv,
            device_id=peer, device_id_type=MESH,
        )

    own_copies = [
        remote(
            hidden.at[:, columns_of(k, y)], tokens.at[k, mine, :],
            send_sem.at[0], x_recv.at[k], x_peer,
        )
        for k in range(n_z)
    ]
    fwd_copies = [
        remote(
            tokens.at[k, mine_far, :], tokens.at[k, mine_far, :],
            send_sem.at[1], x_recv.at[k], x_peer,
        )
        for k in range(n_z)
    ]
    ytok_copies = [
        remote(
            hidden.at[:, columns_of(k, 1 - y)], tokens.at[k, mine_far, :],
            send_sem.at[2], ytok_recv.at[k], y_peer,
        )
        for k in range(n_z)
    ]

    def ygrad(source, first, n):
        span = pl.ds(first, source.shape[1])
        return remote(
            source, grads.at[far, span], send_sem.at[3], ygrad_recv.at[n], y_peer
        )

    ygrad_copies = [
        [ygrad(query_grad.at[:, pl.ds(n * chunk, chunk)], n * chunk, n)]
        for n in range(n_c - 1)
    ] + [[ygrad(key_grad, q_w, n_c - 1), ygrad(value_grad, q_w + k_w, n_c - 1)]]
    head_copies = [
        remote(
            head_out.at[j], head_in.at[j], send_sem.at[4], head_recv.at[j], x_peer
        )
        for j in range(pieces)
    ]
    core_copies = [
        [
            remote(
                core_out.at[k, n], core_in.at[k, n],
                send_sem.at[5], core_recv.at[n if k == 0 else n_c + k - 1], core_peer,
            )
            for n in range(n_c)
        ]
        for k in range(n_z)
    ]
    def place_on(step, below):
        i = below + 1 if order[below][step] > below else below - 1
        if not 0 <= i < n_z or order[below][step] == below:
            return 0
        to = order[below][step]
        if to == i:
            return n_z - 1 if below < i else n_z
        return order[i].index(to)

    z_slot = [pick([place_on(k, i) for i in range(n_z)], z) for k in range(n_z - 1)]
    z_copies = [
        [
            remote(
                z_out.at[k, n], z_in.at[z_slot[k], n],
                send_sem.at[6], z_recv.at[z_slot[k], n],
                (dp + 4 - 8 * down[k], tp),
            )
            for n in range(n_c)
        ]
        for k in range(n_z - 1)
    ]

    def units(source):
        return pl.ds(pl.multiple_of(source * unit, unit), unit)

    fetches = [
        remote(
            source.at[units(dp), :],
            gathered.at[units(dp), pl.ds(first, source.shape[1])],
            send_sem.at[7], plane_recv.at[0], x_peer,
        )
        for source, first in ((w_query, 0), (w_key, q_w), (w_value, q_w + k_w))
    ]
    lend_grads = remote(
        grads.at[theirs, :], own_grads, send_sem.at[8], plane_recv.at[1], x_peer
    )

    def unit_copy(direction, s):
        rows_of = units(dp - 4 * s if direction == 0 else dp + 4 * s)
        return remote(
            gathered.at[rows_of, :], gathered.at[rows_of, :],
            unit_send.at[direction, s], unit_recv.at[direction, s],
            high_peer if direction == 0 else low_peer,
        )

    def to_sibling(source, across):
        remote(
            gathered.at[units(source), :], gathered.at[units(source), :],
            send_sem.at[10], plane_recv.at[3 + across], core_peer,
        ).start()

    def to_plane(source):
        remote(
            gathered.at[units(source), :], gathered.at[units(source), :],
            send_sem.at[9], plane_recv.at[2], y_peer,
        ).start()
        to_sibling(source, 0)

    def landed(whole, semaphore):
        pltpu.make_async_copy(whole, whole, semaphore).wait()

    for copy in own_copies[:1] + fetches:
        copy.start()

    def start_y():
        for copy in ytok_copies[:2]:
            copy.start()
        for copies in ygrad_copies:
            for copy in copies:
                copy.start()
        for copy in ytok_copies[2:]:
            copy.start()

    @pl.when(scout)
    def _():
        start_y()
        around_line(lambda peer: notify(seen_sem, peer))
        pl.semaphore_wait(seen_sem, around)
        notify(go_sem, core_peer)

    @pl.when(jnp.logical_not(scout))
    def _():
        pl.semaphore_wait(go_sem, 1)
        start_y()

    def loaded(index, whole):
        pltpu.make_async_copy(whole, whole, load_sem.at[index]).wait()

    loaded(0, grads.at[near, :])
    loaded(1, weights)

    def head_piece(j):
        columns = pl.ds(own_first + j * width, width)
        head_out[j] = contract_cols(grads[theirs, :], weights[columns, :]).astype(bf16)
        own_head[:, columns] = contract_cols(grads[mine, :], weights[columns, :])
        columns = pl.ds(j * width, width)
        own_head[:, columns] = contract_cols(grads[mine, :], weights[columns, :])

    def block(k, n, which):
        start = pl.multiple_of(which * rows, rows)
        return contract_rows(
            tokens[k, :, pl.ds(start, rows)], grads[:, pl.ds(n * chunk, chunk)]
        )

    def arrive(k):
        if k == 0:
            loaded(2, tokens.at[:, mine, :])
        landed(tokens.at[k, pl.ds(0, group), :], x_recv.at[k])

    def partial(k, n):
        if k == 0:
            landed(grads.at[far, pl.ds(n * chunk, chunk)], ygrad_recv.at[n])
        core_out[k, n] = block(k, n, 1 - core).astype(bf16)
        core_copies[k][n].start()
        total[k, n] = block(k, n, core)

    def sibling_part(k, n):
        if k == 0:
            landed(core_in.at[k, n], core_recv.at[n])
        elif n == 0:
            landed(core_in.at[k], core_recv.at[n_c + k - 1])
        return core_in[k, n].astype(f32)

    def pass_on(k, n, at_line_end):
        def run():
            summed = total[k, n] + sibling_part(k, n)
            if not at_line_end:
                landed(z_in.at[k, n], z_recv.at[k, n])
                summed = summed + z_in[k, n].astype(f32)
            z_out[k, n] = summed.astype(bf16)
            z_copies[k][n].start()

        pl.when(at_end if at_line_end else jnp.logical_not(at_end))(run)

    def finish(n):
        span = pl.ds(n * chunk, chunk)
        final[:, span] = total[last, n] + sibling_part(last, n)

        for slot, edge in ((n_z - 1, at_low), (n_z, at_high)):
            @pl.when(jnp.logical_not(edge))
            def _():
                landed(z_in.at[slot, n], z_recv.at[slot, n])
                final[:, span] += z_in[slot, n].astype(f32)

    def add_heads(j):
        head_copies[j].wait_recv()
        columns = pl.ds(own_first + j * width, width)
        own = own_head[:, columns]
        result[:, columns] = (own + head_in[j].astype(f32)).astype(result.dtype)

    def add_gathered(i, side):
        start = pl.multiple_of((i * 4 + side * 2) * unit, 2 * unit)
        columns = pl.ds(start, 2 * unit)
        other = contract_cols(own_grads[...], gathered[columns, :])
        result[:, columns] = (own_head[:, columns] + other).astype(result.dtype)

    def relay(s):
        for direction, exists, onward, step in (
            (0, z >= s, jnp.logical_not(at_high), -4),
            (1, z <= n_z - 1 - s, jnp.logical_not(at_low), 4),
        ):
            @pl.when(exists)
            def _():
                spread(direction, s, onward, dp + step * s)

    def spread(direction, s, onward, source):
        landed(gathered.at[units(source), :], unit_recv.at[direction, s - 1])
        if s < n_z - 1:
            pl.when(onward)(unit_copy(direction, s).start)
        to_plane(source)

    chunks = range(n_c)
    ready = sent = 0

    def prepare(count):
        nonlocal ready
        for j in range(ready, min(ready + count, pieces)):
            head_piece(j)
        ready = min(ready + count, pieces)

    def send_heads(count):
        nonlocal sent
        for j in range(sent, min(sent + count, ready)):
            head_copies[j].start()
        sent = min(sent + count, ready)

    last = n_z - 1
    in_plane = n_z * unit

    def forward_tokens(k):
        ytok_copies[k].wait_recv()
        fwd_copies[k].start()
        if k < last:
            own_copies[k + 1].start()

    prepare(2)
    forward_tokens(0)
    prepare(1)
    forward_tokens(1)
    lend_grads.start()
    landed(gathered.at[units(dp), :], plane_recv.at[0])
    pl.when(jnp.logical_not(at_high))(unit_copy(0, 0).start)
    pl.when(jnp.logical_not(at_low))(unit_copy(1, 0).start)
    to_plane(dp)
    prepare(pieces)
    arrive(0)
    for n in chunks:
        partial(0, n)
        pass_on(0, n, True)
    relay(1)
    for k in range(1, last):
        forward_tokens(k + 1)
        if k + 1 == last:
            send_heads(pieces)
        arrive(k)
        for n in chunks:
            partial(k, n)
        for n in chunks:
            pass_on(k, n, True)
        for n in chunks:
            pass_on(k - 1, n, False)
        if k + 1 < last:
            relay(k + 1)
    for n in chunks:
        pass_on(last - 1, n, False)
    relay(last)
    arrive(last)
    for n in chunks:
        partial(last, n)
    landed(own_grads, plane_recv.at[1])
    landed(gathered.at[pl.ds(0, in_plane), :], plane_recv.at[3])
    for i in range(n_z):
        add_gathered(i, y)
    for n in chunks[:-1]:
        finish(n)
    landed(gathered.at[pl.ds(0, in_plane), :], plane_recv.at[2])
    for i in range(n_z):
        to_sibling(i * 4 + (1 - y) * 2 + core, 1)
    finish(n_c - 1)
    landed(gathered.at[pl.ds(0, in_plane), :], plane_recv.at[4])
    for i in range(n_z):
        add_gathered(i, 1 - y)
    for j in range(pieces):
        add_heads(j)
    for s in range(n_z - 1):
        for direction, sent_on in (
            (0, jnp.logical_and(z >= s, jnp.logical_not(at_high))),
            (1, jnp.logical_and(z <= n_z - 1 - s, jnp.logical_not(at_low))),
        ):
            @pl.when(sent_on)
            def _():
                landed(gathered.at[units(dp), :], unit_send.at[direction, s])

    sources = (
        tokens.at[:, mine, :], tokens.at[:, mine, :], tokens.at[:, mine, :],
        grads.at[near, :], head_out, core_out, z_out,
        gathered.at[units(dp), :], own_grads, gathered.at[pl.ds(0, n_z * unit), :],
        gathered.at[pl.ds(0, 2 * n_z * unit), :],
    )
    for i, source in enumerate(sources):
        landed(source, send_sem.at[i])


def place(result, final, out_hidden, out_query, out_key, out_value, sem):
    q_w, k_w = out_query.shape[1], out_key.shape[1]
    copies = [
        pltpu.make_async_copy(result, out_hidden, sem.at[0]),
        pltpu.make_async_copy(final.at[:, pl.ds(0, q_w)], out_query, sem.at[1]),
        pltpu.make_async_copy(final.at[:, pl.ds(q_w, k_w)], out_key, sem.at[2]),
        pltpu.make_async_copy(
            final.at[:, pl.ds(q_w + k_w, k_w)], out_value, sem.at[3]
        ),
    ]
    for copy in copies:
        copy.start()
    for copy in copies:
        copy.wait()


def fused(n_dp, hidden, query_grad, key_grad, value_grad, w_query, w_key, w_value):
    half, depth = hidden.shape
    group = query_grad.shape[0]
    q_w, k_w = w_query.shape[1], w_key.shape[1]
    wide = q_w + 2 * k_w
    rows = depth // n_dp
    if q_w % (2 * k_w) or rows % 256 or k_w % 128 or half * 2 != group:
        return local(hidden, query_grad, key_grad, value_grad, w_query, w_key, w_value)
    n_z = n_dp // 4
    n_c = wide // (2 * k_w)
    chunk = 2 * k_w
    pieces = n_z
    width = depth // 2 // pieces
    bf16, f32 = jnp.bfloat16, jnp.float32
    dma = pltpu.SemaphoreType.DMA
    held = pl.pallas_call(
        functools.partial(kernel, n_z, pieces, n_c),
        out_shape=(pltpu.VMEM((half, depth), bf16), pltpu.VMEM((rows, wide), f32)),
        in_specs=[pl.BlockSpec(memory_space=pl.ANY)] * 7,
        out_specs=(pl.BlockSpec(memory_space=pltpu.VMEM),) * 2,
        scratch_shapes=[
            pltpu.VMEM((n_z, 2 * group, 2 * rows), bf16),
            pltpu.VMEM((2 * group, wide), bf16),
            pltpu.VMEM((depth, wide), bf16),
            pltpu.VMEM((pieces, half, width), bf16),
            pltpu.VMEM((pieces, half, width), bf16),
            pltpu.VMEM((n_z, n_c, rows, chunk), bf16),
            pltpu.VMEM((n_z, n_c, rows, chunk), bf16),
            pltpu.VMEM((n_z, n_c, rows, chunk), f32),
            pltpu.VMEM((n_z - 1, n_c, rows, chunk), bf16),
            pltpu.VMEM((n_z + 1, n_c, rows, chunk), bf16),
            pltpu.VMEM((half, depth), f32),
            pltpu.VMEM((depth // 2, wide), bf16),
            pltpu.VMEM((half, wide), bf16),
            dma((3,)), dma((11,)), dma((n_z,)), dma((n_z,)), dma((n_c,)), dma((pieces,)),
            dma((n_c + n_z - 1,)), dma((n_z + 1, n_c)),
            dma((2, n_z - 1)), dma((2, n_z - 1)), dma((5,)),
            pltpu.SemaphoreType.REGULAR, pltpu.SemaphoreType.REGULAR,
        ],
        compiler_params=pltpu.CompilerParams(
            collective_id=0, has_side_effects=True, vmem_limit_bytes=56 * 1024 * 1024
        ),
    )(hidden, query_grad, key_grad, value_grad, w_query, w_key, w_value)
    return pl.pallas_call(
        place,
        out_shape=(
            jax.ShapeDtypeStruct((half, depth), bf16),
            jax.ShapeDtypeStruct((rows, q_w), f32),
            jax.ShapeDtypeStruct((rows, k_w), f32),
            jax.ShapeDtypeStruct((rows, k_w), f32),
        ),
        in_specs=[pl.BlockSpec(memory_space=pltpu.VMEM)] * 2,
        out_specs=(pl.BlockSpec(memory_space=pl.ANY),) * 4,
        scratch_shapes=[dma((4,))],
    )(*[pltpu.with_memory_space_constraint(a, pltpu.VMEM) for a in held])


def solution(mesh):
    placed = (
        P(("dp", "tp"), None),
        P("dp", "tp"),
        P("dp", "tp"),
        P("dp", "tp"),
        P(None, "tp"),
        P(None, "tp"),
        P(None, "tp"),
    )
    n_dp, n_tp = mesh.shape["dp"], mesh.shape["tp"]
    body = local
    if n_tp == 2 and n_dp % 4 == 0 and n_dp > 8:
        body = functools.partial(fused, n_dp)
    return jax.shard_map(
        body,
        mesh=mesh,
        in_specs=placed,
        out_specs=(P(("dp", "tp"), None), P("dp", "tp"), P("dp", "tp"), P("dp", "tp")),
        check_vma=False,
    )
```

```python
import functools

import jax
import jax.numpy as jnp
from jax import lax
from jax.experimental import pallas as pl
from jax.experimental.pallas import tpu as pltpu
from jax.sharding import PartitionSpec as P

MESH = pl.DeviceIdType.MESH


def contract_rows(left, right):
    return lax.dot_general(
        left, right, (((0,), (0,)), ((), ())), preferred_element_type=jnp.float32
    )


def contract_cols(left, right):
    return lax.dot_general(
        left, right, (((1,), (1,)), ((), ())), preferred_element_type=jnp.float32
    )


def local(hidden, query_grad, key_grad, value_grad, w_query, w_key, w_value):
    query_width = w_query.shape[1]
    head_width = w_key.shape[1]
    all_grads = jnp.concatenate((query_grad, key_grad, value_grad), axis=1)
    all_weights = jnp.concatenate((w_query, w_key, w_value), axis=1)
    total = contract_rows(lax.all_gather(hidden, "tp", axis=0, tiled=True), all_grads)
    summed = lax.psum_scatter(
        contract_cols(all_grads, all_weights).astype(jnp.bfloat16),
        "tp",
        scatter_dimension=0,
        tiled=True,
    )
    weight_grad = lax.psum_scatter(
        total.astype(jnp.bfloat16), "dp", scatter_dimension=0, tiled=True
    ).astype(jnp.float32)
    grad_query = weight_grad[:, :query_width]
    grad_key = weight_grad[:, query_width : query_width + head_width]
    grad_value = weight_grad[:, query_width + head_width :]
    return (summed, grad_query, grad_key, grad_value)


def targets(n_z, z):
    near_low = z < n_z - 1 - z
    return sorted(
        range(n_z), key=lambda t: (-abs(t - z), t if near_low else -t)
    )


def pick(values, index):
    chosen = jnp.int32(values[0])
    for i, value in enumerate(values[1:]):
        chosen = jnp.where(index == i + 1, jnp.int32(value), chosen)
    return chosen


def kernel(
    n_z, pieces, n_c,
    hidden, query_grad, key_grad, value_grad, w_query, w_key, w_value,
    result, final,
    tokens, grads, weights, head_out, head_in, core_out, core_in,
    total, z_out, z_in, own_head, gathered, own_grads,
    load_sem, send_sem, x_recv, ytok_recv, ygrad_recv, head_recv, core_recv, z_recv,
    unit_send, unit_recv, plane_recv, across_recv, seen_sem, go_sem,
):
    dp = lax.axis_index("dp")
    tp = lax.axis_index("tp")
    core = lax.rem(dp, 2)
    y = lax.rem(dp // 2, 2)
    z = dp // 4
    half = hidden.shape[0]
    group = query_grad.shape[0]
    q_w = query_grad.shape[1]
    k_w = key_grad.shape[1]
    rows = final.shape[0]
    pair = 2 * rows
    width = hidden.shape[1] // 2 // pieces
    own_first = hidden.shape[1] // 2
    unit = rows // 2
    chunk = 2 * k_w
    bf16, f32 = jnp.bfloat16, jnp.float32

    x_peer = (dp, 1 - tp)
    core_peer = (dp + 1 - 2 * core, tp)
    y_peer = (dp + 2 - 4 * y, tp)
    at_low, at_high = z == 0, z == n_z - 1
    at_end = jnp.logical_or(at_low, at_high)

    order = [targets(n_z, i) for i in range(n_z)]
    target = [pick([order[i][k] for i in range(n_z)], z) for k in range(n_z)]
    down = [jnp.where(target[k] < z, 1, 0) for k in range(n_z)]

    mine = pl.ds(pl.multiple_of(tp * half, half), half)
    theirs = pl.ds(pl.multiple_of((1 - tp) * half, half), half)
    mine_far = pl.ds(pl.multiple_of(group + tp * half, half), half)

    def columns_of(k, side):
        return pl.ds(pl.multiple_of((target[k] * 2 + side) * pair, pair), pair)

    def load(index, source, place):
        pltpu.make_async_copy(source, place, load_sem.at[index]).start()

    near = pl.ds(0, group)
    far = pl.ds(group, group)

    barrier = pltpu.get_barrier_semaphore()

    def greet(peer):
        pl.semaphore_signal(barrier, inc=1, device_id=peer, device_id_type=MESH)

    greet(x_peer)
    scout = core == 0
    low_peer, high_peer = (dp - 4, tp), (dp + 4, tp)
    around = 3 - jnp.where(at_end, 1, 0)

    def around_line(tell):
        tell(y_peer)
        pl.when(jnp.logical_not(at_low))(lambda: tell(low_peer))
        pl.when(jnp.logical_not(at_high))(lambda: tell(high_peer))

    pl.when(scout)(lambda: around_line(greet))
    pl.when(jnp.logical_not(scout))(lambda: greet(core_peer))
    load(0, query_grad, grads.at[near, pl.ds(0, q_w)])
    load(0, key_grad, grads.at[near, pl.ds(q_w, k_w)])
    load(0, value_grad, grads.at[near, pl.ds(q_w + k_w, k_w)])
    load(1, w_query, weights.at[:, pl.ds(0, q_w)])
    load(1, w_key, weights.at[:, pl.ds(q_w, k_w)])
    load(1, w_value, weights.at[:, pl.ds(q_w + k_w, k_w)])
    for k in range(n_z):
        load(2, hidden.at[:, columns_of(k, y)], tokens.at[k, mine, :])

    pl.semaphore_wait(barrier, 1 + jnp.where(scout, 1 + around, 0))

    def notify(semaphore, peer):
        pl.semaphore_signal(semaphore, inc=1, device_id=peer, device_id_type=MESH)

    def remote(source, place, send, recv, peer):
        return pltpu.make_async_remote_copy(
            src_ref=source, dst_ref=place, send_sem=send, recv_sem=recv,
            device_id=peer, device_id_type=MESH,
        )

    own_copies = [
        remote(
            hidden.at[:, columns_of(k, y)], tokens.at[k, mine, :],
            send_sem.at[0], x_recv.at[k], x_peer,
        )
        for k in range(n_z)
    ]
    fwd_copies = [
        remote(
            tokens.at[k, mine_far, :], tokens.at[k, mine_far, :],
            send_sem.at[1], x_recv.at[k], x_peer,
        )
        for k in range(n_z)
    ]
    ytok_copies = [
        remote(
            hidden.at[:, columns_of(k, 1 - y)], tokens.at[k, mine_far, :],
            send_sem.at[2], ytok_recv.at[k], y_peer,
        )
        for k in range(n_z)
    ]

    def ygrad(source, first, n):
        span = pl.ds(first, source.shape[1])
        return remote(
            source, grads.at[far, span], send_sem.at[3], ygrad_recv.at[n], y_peer
        )

    ygrad_copies = [
        [ygrad(query_grad.at[:, pl.ds(n * chunk, chunk)], n * chunk, n)]
        for n in range(n_c - 1)
    ] + [[ygrad(key_grad, q_w, n_c - 1), ygrad(value_grad, q_w + k_w, n_c - 1)]]
    head_copies = [
        remote(
            head_out.at[j], head_in.at[j], send_sem.at[4], head_recv.at[j], x_peer
        )
        for j in range(pieces)
    ]
    core_copies = [
        [
            remote(
                core_out.at[k, n], core_in.at[k, n],
                send_sem.at[5], core_recv.at[n if k == 0 else n_c + k - 1], core_peer,
            )
            for n in range(n_c)
        ]
        for k in range(n_z)
    ]
    def place_on(step, below):
        i = below + 1 if order[below][step] > below else below - 1
        if not 0 <= i < n_z or order[below][step] == below:
            return 0
        to = order[below][step]
        if to == i:
            return n_z - 1 if below < i else n_z
        return order[i].index(to)

    z_slot = [pick([place_on(k, i) for i in range(n_z)], z) for k in range(n_z - 1)]
    z_copies = [
        [
            remote(
                z_out.at[k, n], z_in.at[z_slot[k], n],
                send_sem.at[6], z_recv.at[z_slot[k], n],
                (dp + 4 - 8 * down[k], tp),
            )
            for n in range(n_c)
        ]
        for k in range(n_z - 1)
    ]

    def units(source):
        return pl.ds(pl.multiple_of(source * unit, unit), unit)

    fetches = [
        remote(
            source.at[units(dp), :],
            gathered.at[units(dp), pl.ds(first, source.shape[1])],
            send_sem.at[7], plane_recv.at[0], x_peer,
        )
        for source, first in ((w_query, 0), (w_key, q_w), (w_value, q_w + k_w))
    ]
    lend_grads = remote(
        grads.at[theirs, :], own_grads, send_sem.at[8], plane_recv.at[1], x_peer
    )

    def unit_copy(direction, s):
        rows_of = units(dp - 4 * s if direction == 0 else dp + 4 * s)
        return remote(
            gathered.at[rows_of, :], gathered.at[rows_of, :],
            unit_send.at[direction, s], unit_recv.at[direction, s],
            high_peer if direction == 0 else low_peer,
        )

    def to_sibling(source, across):
        remote(
            gathered.at[units(source), :], gathered.at[units(source), :],
            send_sem.at[10], plane_recv.at[2 + across], core_peer,
        ).start()

    def to_plane(source):
        remote(
            gathered.at[units(source), :], gathered.at[units(source), :],
            send_sem.at[9], across_recv.at[source // 4], y_peer,
        ).start()
        to_sibling(source, 0)

    def landed(whole, semaphore):
        pltpu.make_async_copy(whole, whole, semaphore).wait()

    def loaded(index, whole):
        pltpu.make_async_copy(whole, whole, load_sem.at[index]).wait()

    for copy in own_copies[:1] + fetches:
        copy.start()

    def start_later_y():
        later = ygrad_copies[0] + ytok_copies[1:2]
        for copies in ygrad_copies[1:]:
            later = later + copies
        for copy in later + ytok_copies[2:]:
            copy.start()

    @pl.when(scout)
    def _():
        ytok_copies[0].start()
        around_line(lambda peer: notify(seen_sem, peer))
        pl.semaphore_wait(seen_sem, around)
        notify(go_sem, core_peer)

    @pl.when(jnp.logical_not(scout))
    def _():
        pl.semaphore_wait(go_sem, 1)
        ytok_copies[0].start()
        start_later_y()

    loaded(0, grads.at[near, :])
    loaded(1, weights)

    def head_piece(j):
        columns = pl.ds(own_first + j * width, width)
        head_out[j] = contract_cols(grads[theirs, :], weights[columns, :]).astype(bf16)
        own_head[:, columns] = contract_cols(grads[mine, :], weights[columns, :])
        columns = pl.ds(j * width, width)
        own_head[:, columns] = contract_cols(grads[mine, :], weights[columns, :])

    def block(k, n, which):
        start = pl.multiple_of(which * rows, rows)
        return contract_rows(
            tokens[k, :, pl.ds(start, rows)], grads[:, pl.ds(n * chunk, chunk)]
        )

    def arrive(k):
        if k == 0:
            loaded(2, tokens.at[:, mine, :])
        landed(tokens.at[k, pl.ds(0, group), :], x_recv.at[k])

    def partial(k, n):
        if k == 0:
            landed(grads.at[far, pl.ds(n * chunk, chunk)], ygrad_recv.at[n])
        core_out[k, n] = block(k, n, 1 - core).astype(bf16)
        core_copies[k][n].start()
        total[k, n] = block(k, n, core)

    def sibling_part(k, n):
        if k == 0:
            landed(core_in.at[k, n], core_recv.at[n])
        elif n == 0:
            landed(core_in.at[k], core_recv.at[n_c + k - 1])
        return core_in[k, n].astype(f32)

    def pass_on(k, n, at_line_end):
        def run():
            summed = total[k, n] + sibling_part(k, n)
            if not at_line_end:
                landed(z_in.at[k, n], z_recv.at[k, n])
                summed = summed + z_in[k, n].astype(f32)
            z_out[k, n] = summed.astype(bf16)
            z_copies[k][n].start()

        pl.when(at_end if at_line_end else jnp.logical_not(at_end))(run)

    def finish(n):
        span = pl.ds(n * chunk, chunk)
        final[:, span] = total[last, n] + sibling_part(last, n)

        for slot, edge in ((n_z - 1, at_low), (n_z, at_high)):
            @pl.when(jnp.logical_not(edge))
            def _():
                landed(z_in.at[slot, n], z_recv.at[slot, n])
                final[:, span] += z_in[slot, n].astype(f32)

    def add_heads(j):
        head_copies[j].wait_recv()
        columns = pl.ds(own_first + j * width, width)
        own = own_head[:, columns]
        result[:, columns] = (own + head_in[j].astype(f32)).astype(result.dtype)

    def add_gathered(i, side):
        start = pl.multiple_of((i * 4 + side * 2) * unit, 2 * unit)
        columns = pl.ds(start, 2 * unit)
        other = contract_cols(own_grads[...], gathered[columns, :])
        result[:, columns] = (own_head[:, columns] + other).astype(result.dtype)

    def relay(s):
        for direction, exists, onward, step in (
            (0, z >= s, jnp.logical_not(at_high), -4),
            (1, z <= n_z - 1 - s, jnp.logical_not(at_low), 4),
        ):
            @pl.when(exists)
            def _():
                spread(direction, s, onward, dp + step * s)

    def spread(direction, s, onward, source):
        landed(gathered.at[units(source), :], unit_recv.at[direction, s - 1])
        if s < n_z - 1:
            pl.when(onward)(unit_copy(direction, s).start)
        to_plane(source)

    chunks = range(n_c)
    ready = sent = 0

    def prepare(count):
        nonlocal ready
        for j in range(ready, min(ready + count, pieces)):
            head_piece(j)
        ready = min(ready + count, pieces)

    def send_heads(count):
        nonlocal sent
        for j in range(sent, min(sent + count, ready)):
            head_copies[j].start()
        sent = min(sent + count, ready)

    last = n_z - 1
    in_plane = n_z * unit

    def forward_tokens(k):
        ytok_copies[k].wait_recv()
        fwd_copies[k].start()
        for copy in own_copies[1:3] if k == 0 else own_copies[k + 1 : k + 2]:
            if k != 1:
                copy.start()
        if k == 1:
            lend_grads.start()
        if k == last:
            send_heads(pieces)

    prepare(1)
    pl.when(scout)(start_later_y)
    prepare(1)
    forward_tokens(0)
    prepare(1)
    landed(gathered.at[units(dp), :], plane_recv.at[0])
    pl.when(jnp.logical_not(at_high))(unit_copy(0, 0).start)
    pl.when(jnp.logical_not(at_low))(unit_copy(1, 0).start)
    to_plane(dp)
    prepare(pieces)
    arrive(0)
    partial(0, 0)
    forward_tokens(1)
    pass_on(0, 0, True)
    for n in chunks[1:]:
        if n == n_c - 1:
            relay(1)
        partial(0, n)
        pass_on(0, n, True)
    pass_on(0, 0, False)
    for k in range(1, last):
        forward_tokens(k + 1)
        arrive(k)
        for n in chunks:
            partial(k, n)
        for n in chunks:
            pass_on(k, n, True)
        for n in chunks[1:]:
            pass_on(k - 1, n, False)
        pass_on(k, 0, False)
        if k + 1 < last:
            relay(k + 1)
    for n in chunks[1:]:
        pass_on(last - 1, n, False)
    relay(last)
    arrive(last)
    for n in chunks:
        partial(last, n)
    landed(own_grads, plane_recv.at[1])
    landed(gathered.at[pl.ds(0, in_plane), :], plane_recv.at[2])
    for i in range(n_z):
        add_gathered(i, y)
    for n in chunks[:-1]:
        finish(n)
    for i in reversed(target):
        source = i * 4 + (1 - y) * 2 + core
        landed(gathered.at[units(source), :], across_recv.at[i])
        to_sibling(source, 1)
    finish(n_c - 1)
    landed(gathered.at[pl.ds(0, in_plane), :], plane_recv.at[3])
    for i in range(n_z):
        add_gathered(i, 1 - y)
    for j in range(pieces):
        add_heads(j)
    for s in range(n_z - 1):
        for direction, sent_on in (
            (0, jnp.logical_and(z >= s, jnp.logical_not(at_high))),
            (1, jnp.logical_and(z <= n_z - 1 - s, jnp.logical_not(at_low))),
        ):
            @pl.when(sent_on)
            def _():
                landed(gathered.at[units(dp), :], unit_send.at[direction, s])

    sources = (
        tokens.at[:, mine, :], tokens.at[:, mine, :], tokens.at[:, mine, :],
        grads.at[near, :], head_out, core_out, z_out,
        gathered.at[units(dp), :], own_grads, gathered.at[pl.ds(0, n_z * unit), :],
        gathered.at[pl.ds(0, 2 * n_z * unit), :],
    )
    for i, source in enumerate(sources):
        landed(source, send_sem.at[i])


def place(result, final, out_hidden, out_query, out_key, out_value, sem):
    q_w, k_w = out_query.shape[1], out_key.shape[1]
    copies = [
        pltpu.make_async_copy(result, out_hidden, sem.at[0]),
        pltpu.make_async_copy(final.at[:, pl.ds(0, q_w)], out_query, sem.at[1]),
        pltpu.make_async_copy(final.at[:, pl.ds(q_w, k_w)], out_key, sem.at[2]),
        pltpu.make_async_copy(
            final.at[:, pl.ds(q_w + k_w, k_w)], out_value, sem.at[3]
        ),
    ]
    for copy in copies:
        copy.start()
    for copy in copies:
        copy.wait()


def fused(n_dp, hidden, query_grad, key_grad, value_grad, w_query, w_key, w_value):
    half, depth = hidden.shape
    group = query_grad.shape[0]
    q_w, k_w = w_query.shape[1], w_key.shape[1]
    wide = q_w + 2 * k_w
    rows = depth // n_dp
    if q_w % (2 * k_w) or rows % 256 or k_w % 128 or half * 2 != group:
        return local(hidden, query_grad, key_grad, value_grad, w_query, w_key, w_value)
    n_z = n_dp // 4
    n_c = wide // (2 * k_w)
    chunk = 2 * k_w
    pieces = n_z
    width = depth // 2 // pieces
    bf16, f32 = jnp.bfloat16, jnp.float32
    dma = pltpu.SemaphoreType.DMA
    held = pl.pallas_call(
        functools.partial(kernel, n_z, pieces, n_c),
        out_shape=(pltpu.VMEM((half, depth), bf16), pltpu.VMEM((rows, wide), f32)),
        in_specs=[pl.BlockSpec(memory_space=pl.ANY)] * 7,
        out_specs=(pl.BlockSpec(memory_space=pltpu.VMEM),) * 2,
        scratch_shapes=[
            pltpu.VMEM((n_z, 2 * group, 2 * rows), bf16),
            pltpu.VMEM((2 * group, wide), bf16),
            pltpu.VMEM((depth, wide), bf16),
            pltpu.VMEM((pieces, half, width), bf16),
            pltpu.VMEM((pieces, half, width), bf16),
            pltpu.VMEM((n_z, n_c, rows, chunk), bf16),
            pltpu.VMEM((n_z, n_c, rows, chunk), bf16),
            pltpu.VMEM((n_z, n_c, rows, chunk), f32),
            pltpu.VMEM((n_z - 1, n_c, rows, chunk), bf16),
            pltpu.VMEM((n_z + 1, n_c, rows, chunk), bf16),
            pltpu.VMEM((half, depth), f32),
            pltpu.VMEM((depth // 2, wide), bf16),
            pltpu.VMEM((half, wide), bf16),
            dma((3,)), dma((11,)), dma((n_z,)), dma((n_z,)), dma((n_c,)), dma((pieces,)),
            dma((n_c + n_z - 1,)), dma((n_z + 1, n_c)),
            dma((2, n_z - 1)), dma((2, n_z - 1)), dma((4,)), dma((n_z,)),
            pltpu.SemaphoreType.REGULAR, pltpu.SemaphoreType.REGULAR,
        ],
        compiler_params=pltpu.CompilerParams(
            collective_id=0, has_side_effects=True, vmem_limit_bytes=56 * 1024 * 1024
        ),
    )(hidden, query_grad, key_grad, value_grad, w_query, w_key, w_value)
    return pl.pallas_call(
        place,
        out_shape=(
            jax.ShapeDtypeStruct((half, depth), bf16),
            jax.ShapeDtypeStruct((rows, q_w), f32),
            jax.ShapeDtypeStruct((rows, k_w), f32),
            jax.ShapeDtypeStruct((rows, k_w), f32),
        ),
        in_specs=[pl.BlockSpec(memory_space=pltpu.VMEM)] * 2,
        out_specs=(pl.BlockSpec(memory_space=pl.ANY),) * 4,
        scratch_shapes=[dma((4,))],
    )(*[pltpu.with_memory_space_constraint(a, pltpu.VMEM) for a in held])


def solution(mesh):
    placed = (
        P(("dp", "tp"), None),
        P("dp", "tp"),
        P("dp", "tp"),
        P("dp", "tp"),
        P(None, "tp"),
        P(None, "tp"),
        P(None, "tp"),
    )
    n_dp, n_tp = mesh.shape["dp"], mesh.shape["tp"]
    body = local
    if n_tp == 2 and n_dp % 4 == 0 and n_dp > 8:
        body = functools.partial(fused, n_dp)
    return jax.shard_map(
        body,
        mesh=mesh,
        in_specs=placed,
        out_specs=(P(("dp", "tp"), None), P("dp", "tp"), P("dp", "tp"), P("dp", "tp")),
        check_vma=False,
    )
```

```python
import functools

import jax
import jax.numpy as jnp
from jax import lax
from jax.experimental import pallas as pl
from jax.experimental.pallas import tpu as pltpu
from jax.sharding import PartitionSpec as P

MESH = pl.DeviceIdType.MESH


def contract_rows(left, right):
    return lax.dot_general(
        left, right, (((0,), (0,)), ((), ())), preferred_element_type=jnp.float32
    )


def contract_cols(left, right):
    return lax.dot_general(
        left, right, (((1,), (1,)), ((), ())), preferred_element_type=jnp.float32
    )


def local(hidden, query_grad, key_grad, value_grad, w_query, w_key, w_value):
    query_width = w_query.shape[1]
    head_width = w_key.shape[1]
    all_grads = jnp.concatenate((query_grad, key_grad, value_grad), axis=1)
    all_weights = jnp.concatenate((w_query, w_key, w_value), axis=1)
    total = contract_rows(lax.all_gather(hidden, "tp", axis=0, tiled=True), all_grads)
    summed = lax.psum_scatter(
        contract_cols(all_grads, all_weights).astype(jnp.bfloat16),
        "tp",
        scatter_dimension=0,
        tiled=True,
    )
    weight_grad = lax.psum_scatter(
        total.astype(jnp.bfloat16), "dp", scatter_dimension=0, tiled=True
    ).astype(jnp.float32)
    grad_query = weight_grad[:, :query_width]
    grad_key = weight_grad[:, query_width : query_width + head_width]
    grad_value = weight_grad[:, query_width + head_width :]
    return (summed, grad_query, grad_key, grad_value)


def targets(n_z, z):
    near_low = z < n_z - 1 - z
    return sorted(
        range(n_z), key=lambda t: (-abs(t - z), t if near_low else -t)
    )


def pick(values, index):
    chosen = jnp.int32(values[0])
    for i, value in enumerate(values[1:]):
        chosen = jnp.where(index == i + 1, jnp.int32(value), chosen)
    return chosen


def kernel(
    n_z, pieces, n_c,
    hidden, query_grad, key_grad, value_grad, w_query, w_key, w_value,
    result, final,
    tokens, grads, weights, head_out, head_in, core_out, core_in,
    total, z_out, z_in, own_head, gathered, own_grads,
    load_sem, send_sem, x_recv, ytok_recv, ygrad_recv, head_recv, core_recv, z_recv,
    unit_recv, plane_recv, across_recv, seen_sem, go_sem,
):
    dp = lax.axis_index("dp")
    tp = lax.axis_index("tp")
    core = lax.rem(dp, 2)
    y = lax.rem(dp // 2, 2)
    z = dp // 4
    half = hidden.shape[0]
    group = query_grad.shape[0]
    q_w = query_grad.shape[1]
    k_w = key_grad.shape[1]
    rows = final.shape[0]
    pair = 2 * rows
    width = hidden.shape[1] // 2 // pieces
    own_first = hidden.shape[1] // 2
    unit = rows // 2
    chunk = 2 * k_w
    bf16, f32 = jnp.bfloat16, jnp.float32

    x_peer = (dp, 1 - tp)
    core_peer = (dp + 1 - 2 * core, tp)
    y_peer = (dp + 2 - 4 * y, tp)
    at_low, at_high = z == 0, z == n_z - 1
    at_end = jnp.logical_or(at_low, at_high)

    order = [targets(n_z, i) for i in range(n_z)]
    target = [pick([order[i][k] for i in range(n_z)], z) for k in range(n_z)]
    down = [jnp.where(target[k] < z, 1, 0) for k in range(n_z)]

    mine = pl.ds(pl.multiple_of(tp * half, half), half)
    theirs = pl.ds(pl.multiple_of((1 - tp) * half, half), half)
    mine_far = pl.ds(pl.multiple_of(group + tp * half, half), half)

    def columns_of(k, side):
        return pl.ds(pl.multiple_of((target[k] * 2 + side) * pair, pair), pair)

    def load(index, source, place):
        pltpu.make_async_copy(source, place, load_sem.at[index]).start()

    near = pl.ds(0, group)
    far = pl.ds(group, group)

    barrier = pltpu.get_barrier_semaphore()

    def greet(peer):
        pl.semaphore_signal(barrier, inc=1, device_id=peer, device_id_type=MESH)

    greet(x_peer)
    scout = core == 0
    low_peer, high_peer = (dp - 4, tp), (dp + 4, tp)
    around = 3 - jnp.where(at_end, 1, 0)

    def around_line(tell):
        tell(y_peer)
        pl.when(jnp.logical_not(at_low))(lambda: tell(low_peer))
        pl.when(jnp.logical_not(at_high))(lambda: tell(high_peer))

    pl.when(scout)(lambda: around_line(greet))
    pl.when(jnp.logical_not(scout))(lambda: greet(core_peer))
    load(0, query_grad, grads.at[near, pl.ds(0, q_w)])
    load(0, key_grad, grads.at[near, pl.ds(q_w, k_w)])
    load(0, value_grad, grads.at[near, pl.ds(q_w + k_w, k_w)])
    load(1, w_query, weights.at[:, pl.ds(0, q_w)])
    load(1, w_key, weights.at[:, pl.ds(q_w, k_w)])
    load(1, w_value, weights.at[:, pl.ds(q_w + k_w, k_w)])
    for k in range(n_z):
        load(2, hidden.at[:, columns_of(k, y)], tokens.at[k, mine, :])

    pl.semaphore_wait(barrier, 1 + jnp.where(scout, 1 + around, 0))

    def notify(semaphore, peer):
        pl.semaphore_signal(semaphore, inc=1, device_id=peer, device_id_type=MESH)

    def remote(source, place, send, recv, peer):
        return pltpu.make_async_remote_copy(
            src_ref=source, dst_ref=place, send_sem=send, recv_sem=recv,
            device_id=peer, device_id_type=MESH,
        )

    own_copies = [
        remote(
            hidden.at[:, columns_of(k, y)], tokens.at[k, mine, :],
            send_sem.at[0], x_recv.at[k], x_peer,
        )
        for k in range(n_z)
    ]
    fwd_copies = [
        remote(
            tokens.at[k, mine_far, :], tokens.at[k, mine_far, :],
            send_sem.at[0], x_recv.at[k], x_peer,
        )
        for k in range(n_z)
    ]
    ytok_copies = [
        remote(
            hidden.at[:, columns_of(k, 1 - y)], tokens.at[k, mine_far, :],
            send_sem.at[0], ytok_recv.at[k], y_peer,
        )
        for k in range(n_z)
    ]

    def ygrad(source, first, n):
        span = pl.ds(first, source.shape[1])
        return remote(
            source, grads.at[far, span], send_sem.at[1], ygrad_recv.at[n], y_peer
        )

    ygrad_copies = [
        [ygrad(query_grad.at[:, pl.ds(n * chunk, chunk)], n * chunk, n)]
        for n in range(n_c - 1)
    ] + [[ygrad(key_grad, q_w, n_c - 1), ygrad(value_grad, q_w + k_w, n_c - 1)]]
    head_copies = [
        remote(
            head_out.at[j], head_in.at[j], send_sem.at[0],
            head_recv.at[0 if j < pieces - 1 else 1], x_peer,
        )
        for j in range(pieces)
    ]
    core_copies = [
        [
            remote(
                core_out.at[k, n], core_in.at[k, n],
                send_sem.at[2], core_recv.at[n if k == 0 else n_c + k - 1], core_peer,
            )
            for n in range(n_c)
        ]
        for k in range(n_z)
    ]
    def place_on(step, below):
        i = below + 1 if order[below][step] > below else below - 1
        if not 0 <= i < n_z or order[below][step] == below:
            return 0
        to = order[below][step]
        if to == i:
            return n_z - 1 if below < i else n_z
        return order[i].index(to)

    z_slot = [pick([place_on(k, i) for i in range(n_z)], z) for k in range(n_z - 1)]
    z_copies = [
        [
            remote(
                z_out.at[k, n], z_in.at[z_slot[k], n],
                send_sem.at[3], z_recv.at[z_slot[k], n],
                (dp + 4 - 8 * down[k], tp),
            )
            for n in range(n_c)
        ]
        for k in range(n_z - 1)
    ]

    def units(source):
        return pl.ds(pl.multiple_of(source * unit, unit), unit)

    fetches = [
        remote(
            source.at[units(dp), :],
            gathered.at[units(dp), pl.ds(first, source.shape[1])],
            send_sem.at[1], plane_recv.at[0], x_peer,
        )
        for source, first in ((w_query, 0), (w_key, q_w), (w_value, q_w + k_w))
    ]
    lend_grads = remote(
        grads.at[theirs, :], own_grads, send_sem.at[1], plane_recv.at[1], x_peer
    )

    def unit_copy(direction, s):
        rows_of = units(dp - 4 * s if direction == 0 else dp + 4 * s)
        return remote(
            gathered.at[rows_of, :], gathered.at[rows_of, :],
            send_sem.at[4], unit_recv.at[z - s if direction == 0 else z + s],
            high_peer if direction == 0 else low_peer,
        )

    def to_sibling(source, across):
        remote(
            gathered.at[units(source), :], gathered.at[units(source), :],
            send_sem.at[1], plane_recv.at[2 + across], core_peer,
        ).start()

    def to_plane(source):
        remote(
            gathered.at[units(source), :], gathered.at[units(source), :],
            send_sem.at[1], across_recv.at[source // 4], y_peer,
        ).start()
        to_sibling(source, 0)

    def landed(whole, semaphore):
        pltpu.make_async_copy(whole, whole, semaphore).wait()

    def loaded(index, whole):
        pltpu.make_async_copy(whole, whole, load_sem.at[index]).wait()

    for copy in fetches + own_copies[:1]:
        copy.start()

    def start_later_y():
        later = ygrad_copies[0] + ytok_copies[1:2]
        for copies in ygrad_copies[1:]:
            later = later + copies
        for copy in later + ytok_copies[2:]:
            copy.start()

    @pl.when(scout)
    def _():
        ytok_copies[0].start()
        around_line(lambda peer: notify(seen_sem, peer))
        pl.semaphore_wait(seen_sem, around)
        notify(go_sem, core_peer)

    @pl.when(jnp.logical_not(scout))
    def _():
        pl.semaphore_wait(go_sem, 1)
        ytok_copies[0].start()
        start_later_y()

    loaded(0, grads.at[near, :])
    loaded(1, weights)

    def head_piece(j):
        columns = pl.ds(own_first + j * width, width)
        head_out[j] = contract_cols(grads[theirs, :], weights[columns, :]).astype(bf16)
        own_head[:, columns] = contract_cols(grads[mine, :], weights[columns, :])
        columns = pl.ds(j * width, width)
        own_head[:, columns] = contract_cols(grads[mine, :], weights[columns, :])

    def block(k, n, which):
        start = pl.multiple_of(which * rows, rows)
        return contract_rows(
            tokens[k, :, pl.ds(start, rows)], grads[:, pl.ds(n * chunk, chunk)]
        )

    def arrive(k):
        if k == 0:
            loaded(2, tokens.at[:, mine, :])
        landed(tokens.at[k, pl.ds(0, group), :], x_recv.at[k])

    def partial(k, n):
        if k == 0:
            landed(grads.at[far, pl.ds(n * chunk, chunk)], ygrad_recv.at[n])
        core_out[k, n] = block(k, n, 1 - core).astype(bf16)
        core_copies[k][n].start()
        total[k, n] = block(k, n, core)

    def sibling_part(k, n):
        if k == 0:
            landed(core_in.at[k, n], core_recv.at[n])
        elif n == 0:
            landed(core_in.at[k], core_recv.at[n_c + k - 1])
        return core_in[k, n].astype(f32)

    def pass_on(k, n, at_line_end):
        def run():
            summed = total[k, n] + sibling_part(k, n)
            if not at_line_end:
                landed(z_in.at[k, n], z_recv.at[k, n])
                summed = summed + z_in[k, n].astype(f32)
            z_out[k, n] = summed.astype(bf16)
            z_copies[k][n].start()

        pl.when(at_end if at_line_end else jnp.logical_not(at_end))(run)

    def finish(n):
        span = pl.ds(n * chunk, chunk)
        final[:, span] = total[last, n] + sibling_part(last, n)

        for slot, edge in ((n_z - 1, at_low), (n_z, at_high)):
            @pl.when(jnp.logical_not(edge))
            def _():
                landed(z_in.at[slot, n], z_recv.at[slot, n])
                final[:, span] += z_in[slot, n].astype(f32)

    def add_heads(j):
        if j == 0:
            landed(head_in.at[pl.ds(0, pieces - 1)], head_recv.at[0])
        elif j == pieces - 1:
            landed(head_in.at[j], head_recv.at[1])
        columns = pl.ds(own_first + j * width, width)
        own = own_head[:, columns]
        result[:, columns] = (own + head_in[j].astype(f32)).astype(result.dtype)

    def add_gathered(i, side):
        start = pl.multiple_of((i * 4 + side * 2) * unit, 2 * unit)
        columns = pl.ds(start, 2 * unit)
        other = contract_cols(own_grads[...], gathered[columns, :])
        result[:, columns] = (own_head[:, columns] + other).astype(result.dtype)

    def relay(s):
        for direction, exists, onward, step in (
            (0, z >= s, jnp.logical_not(at_high), -4),
            (1, z <= n_z - 1 - s, jnp.logical_not(at_low), 4),
        ):
            @pl.when(exists)
            def _():
                spread(direction, s, onward, dp + step * s)

    def spread(direction, s, onward, source):
        landed(gathered.at[units(source), :], unit_recv.at[z - s if direction == 0 else z + s])
        if s < n_z - 1:
            pl.when(onward)(unit_copy(direction, s).start)
        to_plane(source)

    chunks = range(n_c)
    ready = sent = 0

    def prepare(count):
        nonlocal ready
        for j in range(ready, min(ready + count, pieces)):
            head_piece(j)
        ready = min(ready + count, pieces)

    def send_heads(count):
        nonlocal sent
        for j in range(sent, min(sent + count, ready)):
            head_copies[j].start()
        sent = min(sent + count, ready)

    last = n_z - 1
    in_plane = n_z * unit

    def forward_tokens(k):
        ytok_copies[k].wait_recv()
        fwd_copies[k].start()
        for copy in own_copies[1:3] if k == 0 else own_copies[k + 1 : k + 2]:
            if k != 1:
                copy.start()
        if k == 1:
            lend_grads.start()
        if k == last:
            send_heads(pieces)

    prepare(1)
    pl.when(scout)(start_later_y)
    prepare(1)
    forward_tokens(0)
    landed(gathered.at[units(dp), :], plane_recv.at[0])
    pl.when(jnp.logical_not(at_high))(unit_copy(0, 0).start)
    pl.when(jnp.logical_not(at_low))(unit_copy(1, 0).start)
    to_plane(dp)
    prepare(2)
    arrive(0)
    partial(0, 0)
    forward_tokens(1)
    pass_on(0, 0, True)
    for n in chunks[1:]:
        if n == n_c - 1:
            relay(1)
        partial(0, n)
        pass_on(0, n, True)
    pass_on(0, 0, False)
    for k in range(1, last):
        forward_tokens(k + 1)
        arrive(k)
        for n in chunks:
            partial(k, n)
        for n in chunks:
            pass_on(k, n, True)
        for n in chunks[1:]:
            pass_on(k - 1, n, False)
        pass_on(k, 0, False)
        if k + 1 < last:
            relay(k + 1)
    for n in chunks[1:]:
        pass_on(last - 1, n, False)
    relay(last)
    arrive(last)
    for n in chunks:
        partial(last, n)
    landed(own_grads, plane_recv.at[1])
    landed(gathered.at[pl.ds(0, in_plane), :], plane_recv.at[2])
    for i in range(n_z):
        add_gathered(i, y)
    for n in chunks[:-1]:
        finish(n)
    for i in reversed(target):
        source = i * 4 + (1 - y) * 2 + core
        landed(gathered.at[units(source), :], across_recv.at[i])
        to_sibling(source, 1)
    finish(n_c - 1)
    landed(gathered.at[pl.ds(0, in_plane), :], plane_recv.at[3])
    for i in range(n_z):
        add_gathered(i, 1 - y)
    for j in range(pieces):
        add_heads(j)
    units_sent = gathered.at[pl.ds(0, (3 * n_z + 4) * unit), :]
    sources = (tokens, units_sent, core_out, z_out)
    for i, source in enumerate(sources):
        landed(source, send_sem.at[i])
    for count, here in ((1, at_end), (n_z + 1, jnp.logical_not(at_end))):
        pl.when(here)(
            lambda: landed(gathered.at[pl.ds(0, count * unit), :], send_sem.at[4])
        )


def place(result, final, out_hidden, out_query, out_key, out_value, sem):
    q_w, k_w = out_query.shape[1], out_key.shape[1]
    copies = [
        pltpu.make_async_copy(result, out_hidden, sem.at[0]),
        pltpu.make_async_copy(final.at[:, pl.ds(0, q_w)], out_query, sem.at[1]),
        pltpu.make_async_copy(final.at[:, pl.ds(q_w, k_w)], out_key, sem.at[2]),
        pltpu.make_async_copy(
            final.at[:, pl.ds(q_w + k_w, k_w)], out_value, sem.at[3]
        ),
    ]
    for copy in copies:
        copy.start()
    for copy in copies:
        copy.wait()


def fused(n_dp, hidden, query_grad, key_grad, value_grad, w_query, w_key, w_value):
    half, depth = hidden.shape
    group = query_grad.shape[0]
    q_w, k_w = w_query.shape[1], w_key.shape[1]
    wide = q_w + 2 * k_w
    rows = depth // n_dp
    if q_w % (2 * k_w) or rows != group or rows % 256 or k_w % 128:
        return local(hidden, query_grad, key_grad, value_grad, w_query, w_key, w_value)
    n_z = n_dp // 4
    n_c = wide // (2 * k_w)
    chunk = 2 * k_w
    pieces = n_z
    width = depth // 2 // pieces
    bf16, f32 = jnp.bfloat16, jnp.float32
    dma = pltpu.SemaphoreType.DMA
    held = pl.pallas_call(
        functools.partial(kernel, n_z, pieces, n_c),
        out_shape=(pltpu.VMEM((half, depth), bf16), pltpu.VMEM((rows, wide), f32)),
        in_specs=[pl.BlockSpec(memory_space=pl.ANY)] * 7,
        out_specs=(pl.BlockSpec(memory_space=pltpu.VMEM),) * 2,
        scratch_shapes=[
            pltpu.VMEM((n_z, 2 * group, 2 * rows), bf16),
            pltpu.VMEM((2 * group, wide), bf16),
            pltpu.VMEM((depth, wide), bf16),
            pltpu.VMEM((pieces, half, width), bf16),
            pltpu.VMEM((pieces, half, width), bf16),
            pltpu.VMEM((n_z, n_c, rows, chunk), bf16),
            pltpu.VMEM((n_z, n_c, rows, chunk), bf16),
            pltpu.VMEM((n_z, n_c, rows, chunk), f32),
            pltpu.VMEM((n_z - 1, n_c, rows, chunk), bf16),
            pltpu.VMEM((n_z + 1, n_c, rows, chunk), bf16),
            pltpu.VMEM((half, depth), f32),
            pltpu.VMEM((depth // 2, wide), bf16),
            pltpu.VMEM((half, wide), bf16),
            dma((3,)), dma((5,)), dma((n_z,)), dma((n_z,)), dma((n_c,)), dma((2,)),
            dma((n_c + n_z - 1,)), dma((n_z + 1, n_c)),
            dma((n_z,)), dma((4,)), dma((n_z,)),
            pltpu.SemaphoreType.REGULAR, pltpu.SemaphoreType.REGULAR,
        ],
        compiler_params=pltpu.CompilerParams(
            collective_id=0, has_side_effects=True, vmem_limit_bytes=56 * 1024 * 1024
        ),
    )(hidden, query_grad, key_grad, value_grad, w_query, w_key, w_value)
    return pl.pallas_call(
        place,
        out_shape=(
            jax.ShapeDtypeStruct((half, depth), bf16),
            jax.ShapeDtypeStruct((rows, q_w), f32),
            jax.ShapeDtypeStruct((rows, k_w), f32),
            jax.ShapeDtypeStruct((rows, k_w), f32),
        ),
        in_specs=[pl.BlockSpec(memory_space=pltpu.VMEM)] * 2,
        out_specs=(pl.BlockSpec(memory_space=pl.ANY),) * 4,
        scratch_shapes=[dma((4,))],
    )(*[pltpu.with_memory_space_constraint(a, pltpu.VMEM) for a in held])


def solution(mesh):
    placed = (
        P(("dp", "tp"), None),
        P("dp", "tp"),
        P("dp", "tp"),
        P("dp", "tp"),
        P(None, "tp"),
        P(None, "tp"),
        P(None, "tp"),
    )
    n_dp, n_tp = mesh.shape["dp"], mesh.shape["tp"]
    body = local
    if n_tp == 2 and n_dp % 4 == 0 and n_dp > 12:
        body = functools.partial(fused, n_dp)
    return jax.shard_map(
        body,
        mesh=mesh,
        in_specs=placed,
        out_specs=(P(("dp", "tp"), None), P("dp", "tp"), P("dp", "tp"), P("dp", "tp")),
        check_vma=False,
    )
```

```python
import functools

import jax
import jax.numpy as jnp
from jax import lax
from jax.experimental import pallas as pl
from jax.experimental.pallas import tpu as pltpu
from jax.sharding import PartitionSpec as P

MESH = pl.DeviceIdType.MESH


def contract_rows(left, right):
    return lax.dot_general(
        left, right, (((0,), (0,)), ((), ())), preferred_element_type=jnp.float32
    )


def contract_cols(left, right):
    return lax.dot_general(
        left, right, (((1,), (1,)), ((), ())), preferred_element_type=jnp.float32
    )


def local(hidden, query_grad, key_grad, value_grad, w_query, w_key, w_value):
    query_width = w_query.shape[1]
    head_width = w_key.shape[1]
    all_grads = jnp.concatenate((query_grad, key_grad, value_grad), axis=1)
    all_weights = jnp.concatenate((w_query, w_key, w_value), axis=1)
    total = contract_rows(lax.all_gather(hidden, "tp", axis=0, tiled=True), all_grads)
    summed = lax.psum_scatter(
        contract_cols(all_grads, all_weights).astype(jnp.bfloat16),
        "tp",
        scatter_dimension=0,
        tiled=True,
    )
    weight_grad = lax.psum_scatter(
        total.astype(jnp.bfloat16), "dp", scatter_dimension=0, tiled=True
    ).astype(jnp.float32)
    grad_query = weight_grad[:, :query_width]
    grad_key = weight_grad[:, query_width : query_width + head_width]
    grad_value = weight_grad[:, query_width + head_width :]
    return (summed, grad_query, grad_key, grad_value)


def targets(n_z, z):
    near_low = z < n_z - 1 - z
    return sorted(
        range(n_z), key=lambda t: (-abs(t - z), t if near_low else -t)
    )


def pick(values, index):
    chosen = jnp.int32(values[0])
    for i, value in enumerate(values[1:]):
        chosen = jnp.where(index == i + 1, jnp.int32(value), chosen)
    return chosen


def kernel(
    n_z, pieces, n_c,
    hidden, query_grad, key_grad, value_grad, w_query, w_key, w_value,
    result, final,
    tokens, grads, weights, head_out, head_in, core_out, core_in,
    total, z_out, z_in, own_head, gathered, own_grads,
    head_sem,
):
    half = hidden.shape[0]
    own_first = hidden.shape[1] // 2
    width = own_first // pieces
    dma = pltpu.SemaphoreType.DMA
    regular = pltpu.SemaphoreType.REGULAR

    def landed(whole, semaphore):
        pltpu.make_async_copy(whole, whole, semaphore).wait()

    def add_heads(j):
        columns = pl.ds(own_first + j * width, width)
        own = own_head[:, columns]
        result[:, columns] = (own + head_in[j].astype(jnp.float32)).astype(result.dtype)

    def scope(
        load_sem, send_sem, x_recv, ytok_recv, ygrad_recv, core_recv, z_recv,
        unit_recv, plane_recv, across_recv, seen_sem, go_sem,
    ):
        dp = lax.axis_index("dp")
        tp = lax.axis_index("tp")
        core = lax.rem(dp, 2)
        y = lax.rem(dp // 2, 2)
        z = dp // 4
        half = hidden.shape[0]
        group = query_grad.shape[0]
        q_w = query_grad.shape[1]
        k_w = key_grad.shape[1]
        rows = final.shape[0]
        pair = 2 * rows
        width = hidden.shape[1] // 2 // pieces
        own_first = hidden.shape[1] // 2
        unit = rows // 2
        chunk = 2 * k_w
        bf16, f32 = jnp.bfloat16, jnp.float32

        x_peer = (dp, 1 - tp)
        core_peer = (dp + 1 - 2 * core, tp)
        y_peer = (dp + 2 - 4 * y, tp)
        at_low, at_high = z == 0, z == n_z - 1
        at_end = jnp.logical_or(at_low, at_high)

        order = [targets(n_z, i) for i in range(n_z)]
        target = [pick([order[i][k] for i in range(n_z)], z) for k in range(n_z)]
        down = [jnp.where(target[k] < z, 1, 0) for k in range(n_z)]

        mine = pl.ds(pl.multiple_of(tp * half, half), half)
        theirs = pl.ds(pl.multiple_of((1 - tp) * half, half), half)
        mine_far = pl.ds(pl.multiple_of(group + tp * half, half), half)

        def columns_of(k, side):
            return pl.ds(pl.multiple_of((target[k] * 2 + side) * pair, pair), pair)

        def load(index, source, place):
            pltpu.make_async_copy(source, place, load_sem.at[index]).start()

        near = pl.ds(0, group)
        far = pl.ds(group, group)

        barrier = pltpu.get_barrier_semaphore()

        def greet(peer):
            pl.semaphore_signal(barrier, inc=1, device_id=peer, device_id_type=MESH)

        greet(x_peer)
        scout = core == 0
        low_peer, high_peer = (dp - 4, tp), (dp + 4, tp)
        around = 3 - jnp.where(at_end, 1, 0)

        def around_line(tell):
            tell(y_peer)
            pl.when(jnp.logical_not(at_low))(lambda: tell(low_peer))
            pl.when(jnp.logical_not(at_high))(lambda: tell(high_peer))

        pl.when(scout)(lambda: around_line(greet))
        pl.when(jnp.logical_not(scout))(lambda: greet(core_peer))
        load(0, query_grad, grads.at[near, pl.ds(0, q_w)])
        load(0, key_grad, grads.at[near, pl.ds(q_w, k_w)])
        load(0, value_grad, grads.at[near, pl.ds(q_w + k_w, k_w)])
        load(1, w_query, weights.at[:, pl.ds(0, q_w)])
        load(1, w_key, weights.at[:, pl.ds(q_w, k_w)])
        load(1, w_value, weights.at[:, pl.ds(q_w + k_w, k_w)])
        for k in range(n_z):
            load(2, hidden.at[:, columns_of(k, y)], tokens.at[k, mine, :])

        pl.semaphore_wait(barrier, 1 + jnp.where(scout, 1 + around, 0))

        def notify(semaphore, peer):
            pl.semaphore_signal(semaphore, inc=1, device_id=peer, device_id_type=MESH)

        def remote(source, place, send, recv, peer):
            return pltpu.make_async_remote_copy(
                src_ref=source, dst_ref=place, send_sem=send, recv_sem=recv,
                device_id=peer, device_id_type=MESH,
            )

        own_copies = [
            remote(
                hidden.at[:, columns_of(k, y)], tokens.at[k, mine, :],
                send_sem.at[0], x_recv.at[k], x_peer,
            )
            for k in range(n_z)
        ]
        fwd_copies = [
            remote(
                tokens.at[k, mine_far, :], tokens.at[k, mine_far, :],
                send_sem.at[0], x_recv.at[k], x_peer,
            )
            for k in range(n_z)
        ]
        ytok_copies = [
            remote(
                hidden.at[:, columns_of(k, 1 - y)], tokens.at[k, mine_far, :],
                send_sem.at[0], ytok_recv.at[k], y_peer,
            )
            for k in range(n_z)
        ]

        def ygrad(source, first, n):
            span = pl.ds(first, source.shape[1])
            return remote(
                source, grads.at[far, span], send_sem.at[1], ygrad_recv.at[n], y_peer
            )

        ygrad_copies = [
            [ygrad(query_grad.at[:, pl.ds(n * chunk, chunk)], n * chunk, n)]
            for n in range(n_c - 1)
        ] + [[ygrad(key_grad, q_w, n_c - 1), ygrad(value_grad, q_w + k_w, n_c - 1)]]
        head_copies = [
            remote(
                head_out.at[j], head_in.at[j], head_sem.at[0],
                head_sem.at[1 if j < pieces - 1 else 2], x_peer,
            )
            for j in range(pieces)
        ]
        core_copies = [
            [
                remote(
                    core_out.at[k, n], core_in.at[k, n],
                    send_sem.at[2], core_recv.at[n if k == 0 else n_c + k - 1], core_peer,
                )
                for n in range(n_c)
            ]
            for k in range(n_z)
        ]
        def place_on(step, below):
            i = below + 1 if order[below][step] > below else below - 1
            if not 0 <= i < n_z or order[below][step] == below:
                return 0
            to = order[below][step]
            if to == i:
                return n_z - 1 if below < i else n_z
            return order[i].index(to)

        z_slot = [pick([place_on(k, i) for i in range(n_z)], z) for k in range(n_z - 1)]
        z_copies = [
            [
                remote(
                    z_out.at[k, n], z_in.at[z_slot[k], n],
                    send_sem.at[3], z_recv.at[z_slot[k], n],
                    (dp + 4 - 8 * down[k], tp),
                )
                for n in range(n_c)
            ]
            for k in range(n_z - 1)
        ]

        def units(source):
            return pl.ds(pl.multiple_of(source * unit, unit), unit)

        fetches = [
            remote(
                source.at[units(dp), :],
                gathered.at[units(dp), pl.ds(first, source.shape[1])],
                send_sem.at[1], plane_recv.at[0], x_peer,
            )
            for source, first in ((w_query, 0), (w_key, q_w), (w_value, q_w + k_w))
        ]
        lend_grads = remote(
            grads.at[theirs, :], own_grads, send_sem.at[1], plane_recv.at[1], x_peer
        )

        def unit_copy(direction, s):
            rows_of = units(dp - 4 * s if direction == 0 else dp + 4 * s)
            return remote(
                gathered.at[rows_of, :], gathered.at[rows_of, :],
                send_sem.at[4], unit_recv.at[z - s if direction == 0 else z + s],
                high_peer if direction == 0 else low_peer,
            )

        def to_sibling(source, across):
            remote(
                gathered.at[units(source), :], gathered.at[units(source), :],
                send_sem.at[1], plane_recv.at[2 + across], core_peer,
            ).start()

        def to_plane(source):
            remote(
                gathered.at[units(source), :], gathered.at[units(source), :],
                send_sem.at[1], across_recv.at[source // 4], y_peer,
            ).start()
            to_sibling(source, 0)

        def loaded(index, whole):
            pltpu.make_async_copy(whole, whole, load_sem.at[index]).wait()

        for copy in fetches + own_copies[:1]:
            copy.start()

        def start_later_y():
            later = ygrad_copies[0] + ytok_copies[1:2]
            for copies in ygrad_copies[1:]:
                later = later + copies
            for copy in later + ytok_copies[2:]:
                copy.start()

        @pl.when(scout)
        def _():
            ytok_copies[0].start()
            around_line(lambda peer: notify(seen_sem, peer))
            pl.semaphore_wait(seen_sem, around)
            notify(go_sem, core_peer)

        @pl.when(jnp.logical_not(scout))
        def _():
            pl.semaphore_wait(go_sem, 1)
            ytok_copies[0].start()
            start_later_y()

        loaded(0, grads.at[near, :])
        loaded(1, weights)

        def head_piece(j):
            columns = pl.ds(own_first + j * width, width)
            head_out[j] = contract_cols(grads[theirs, :], weights[columns, :]).astype(bf16)
            own_head[:, columns] = contract_cols(grads[mine, :], weights[columns, :])
            columns = pl.ds(j * width, width)
            own_head[:, columns] = contract_cols(grads[mine, :], weights[columns, :])

        def block(k, n, which):
            start = pl.multiple_of(which * rows, rows)
            return contract_rows(
                tokens[k, :, pl.ds(start, rows)], grads[:, pl.ds(n * chunk, chunk)]
            )

        def arrive(k):
            if k == 0:
                loaded(2, tokens.at[:, mine, :])
            landed(tokens.at[k, pl.ds(0, group), :], x_recv.at[k])

        def partial(k, n):
            if k == 0:
                landed(grads.at[far, pl.ds(n * chunk, chunk)], ygrad_recv.at[n])
            core_out[k, n] = block(k, n, 1 - core).astype(bf16)
            core_copies[k][n].start()
            total[k, n] = block(k, n, core)

        def sibling_part(k, n):
            if k == 0:
                landed(core_in.at[k, n], core_recv.at[n])
            elif n == 0:
                landed(core_in.at[k], core_recv.at[n_c + k - 1])
            return core_in[k, n].astype(f32)

        def pass_on(k, n, at_line_end):
            def run():
                summed = total[k, n] + sibling_part(k, n)
                if not at_line_end:
                    landed(z_in.at[k, n], z_recv.at[k, n])
                    summed = summed + z_in[k, n].astype(f32)
                z_out[k, n] = summed.astype(bf16)
                z_copies[k][n].start()

            pl.when(at_end if at_line_end else jnp.logical_not(at_end))(run)

        def finish(n):
            span = pl.ds(n * chunk, chunk)
            final[:, span] = total[last, n] + sibling_part(last, n)

            for slot, edge in ((n_z - 1, at_low), (n_z, at_high)):
                @pl.when(jnp.logical_not(edge))
                def _():
                    landed(z_in.at[slot, n], z_recv.at[slot, n])
                    final[:, span] += z_in[slot, n].astype(f32)

        def add_gathered(i, side):
            start = pl.multiple_of((i * 4 + side * 2) * unit, 2 * unit)
            columns = pl.ds(start, 2 * unit)
            other = contract_cols(own_grads[...], gathered[columns, :])
            result[:, columns] = (own_head[:, columns] + other).astype(result.dtype)

        def relay(s):
            for direction, exists, onward, step in (
                (0, z >= s, jnp.logical_not(at_high), -4),
                (1, z <= n_z - 1 - s, jnp.logical_not(at_low), 4),
            ):
                @pl.when(exists)
                def _():
                    spread(direction, s, onward, dp + step * s)

        def spread(direction, s, onward, source):
            landed(gathered.at[units(source), :], unit_recv.at[z - s if direction == 0 else z + s])
            if s < n_z - 1:
                pl.when(onward)(unit_copy(direction, s).start)
            to_plane(source)

        chunks = range(n_c)
        ready = sent = 0

        def prepare(count):
            nonlocal ready
            for j in range(ready, min(ready + count, pieces)):
                head_piece(j)
            ready = min(ready + count, pieces)

        def send_heads(count):
            nonlocal sent
            for j in range(sent, min(sent + count, ready)):
                head_copies[j].start()
            sent = min(sent + count, ready)

        last = n_z - 1
        in_plane = n_z * unit

        def forward_tokens(k):
            ytok_copies[k].wait_recv()
            fwd_copies[k].start()
            for copy in own_copies[1:3] if k == 0 else own_copies[k + 1 : k + 2]:
                if k != 1:
                    copy.start()
            if k == 1:
                lend_grads.start()
            if k == last:
                send_heads(pieces)

        prepare(1)
        pl.when(scout)(start_later_y)
        prepare(1)
        forward_tokens(0)
        landed(gathered.at[units(dp), :], plane_recv.at[0])
        pl.when(jnp.logical_not(at_high))(unit_copy(0, 0).start)
        pl.when(jnp.logical_not(at_low))(unit_copy(1, 0).start)
        to_plane(dp)
        prepare(2)
        arrive(0)
        partial(0, 0)
        forward_tokens(1)
        pass_on(0, 0, True)
        for n in chunks[1:]:
            if n == n_c - 1:
                relay(1)
            partial(0, n)
            pass_on(0, n, True)
        pass_on(0, 0, False)
        for k in range(1, last):
            forward_tokens(k + 1)
            arrive(k)
            for n in chunks:
                partial(k, n)
            for n in chunks:
                pass_on(k, n, True)
            for n in chunks[1:]:
                pass_on(k - 1, n, False)
            pass_on(k, 0, False)
            if k + 1 < last:
                relay(k + 1)
        for n in chunks[1:]:
            pass_on(last - 1, n, False)
        relay(last)
        arrive(last)
        for n in chunks:
            partial(last, n)
        landed(own_grads, plane_recv.at[1])
        landed(gathered.at[pl.ds(0, in_plane), :], plane_recv.at[2])
        for i in range(n_z):
            add_gathered(i, y)
        for n in chunks[:-1]:
            finish(n)
        for i in reversed(target):
            source = i * 4 + (1 - y) * 2 + core
            landed(gathered.at[units(source), :], across_recv.at[i])
            to_sibling(source, 1)
        finish(n_c - 1)
        landed(gathered.at[pl.ds(0, in_plane), :], plane_recv.at[3])
        for i in range(n_z):
            add_gathered(i, 1 - y)
        units_sent = gathered.at[pl.ds(0, (3 * n_z + 4) * unit), :]
        sources = (tokens.at[:, pl.ds(0, 3 * half), :], units_sent, core_out, z_out)
        for i, source in enumerate(sources):
            landed(source, send_sem.at[i])
        for count, here in ((1, at_end), (n_z + 1, jnp.logical_not(at_end))):
            pl.when(here)(
                lambda: landed(gathered.at[pl.ds(0, count * unit), :], send_sem.at[4])
            )

    pl.run_scoped(
        scope,
        dma((3,)), dma((5,)), dma((n_z,)), dma((n_z,)), dma((n_c,)),
        dma((n_c + n_z - 1,)), dma((n_z + 1, n_c)),
        dma((n_z,)), dma((4,)), dma((n_z,)), regular, regular,
    )
    landed(head_in.at[pl.ds(0, pieces - 1)], head_sem.at[1])
    for j in range(pieces - 1):
        add_heads(j)
    landed(head_in.at[pieces - 1], head_sem.at[2])
    add_heads(pieces - 1)
    landed(head_out, head_sem.at[0])


def place(result, final, out_hidden, out_query, out_key, out_value, sem):
    q_w, k_w = out_query.shape[1], out_key.shape[1]
    copies = [
        pltpu.make_async_copy(result, out_hidden, sem.at[0]),
        pltpu.make_async_copy(final.at[:, pl.ds(0, q_w)], out_query, sem.at[1]),
        pltpu.make_async_copy(final.at[:, pl.ds(q_w, k_w)], out_key, sem.at[2]),
        pltpu.make_async_copy(
            final.at[:, pl.ds(q_w + k_w, k_w)], out_value, sem.at[3]
        ),
    ]
    for copy in copies:
        copy.start()
    for copy in copies:
        copy.wait()


def fused(n_dp, hidden, query_grad, key_grad, value_grad, w_query, w_key, w_value):
    half, depth = hidden.shape
    group = query_grad.shape[0]
    q_w, k_w = w_query.shape[1], w_key.shape[1]
    wide = q_w + 2 * k_w
    rows = depth // n_dp
    if q_w % (2 * k_w) or rows != group or rows % 256 or k_w % 128:
        return local(hidden, query_grad, key_grad, value_grad, w_query, w_key, w_value)
    n_z = n_dp // 4
    n_c = wide // (2 * k_w)
    chunk = 2 * k_w
    pieces = n_z
    width = depth // 2 // pieces
    bf16, f32 = jnp.bfloat16, jnp.float32
    dma = pltpu.SemaphoreType.DMA
    held = pl.pallas_call(
        functools.partial(kernel, n_z, pieces, n_c),
        out_shape=(pltpu.VMEM((half, depth), bf16), pltpu.VMEM((rows, wide), f32)),
        in_specs=[pl.BlockSpec(memory_space=pl.ANY)] * 7,
        out_specs=(pl.BlockSpec(memory_space=pltpu.VMEM),) * 2,
        scratch_shapes=[
            pltpu.VMEM((n_z, 2 * group, 2 * rows), bf16),
            pltpu.VMEM((2 * group, wide), bf16),
            pltpu.VMEM((depth, wide), bf16),
            pltpu.VMEM((pieces, half, width), bf16),
            pltpu.VMEM((pieces, half, width), bf16),
            pltpu.VMEM((n_z, n_c, rows, chunk), bf16),
            pltpu.VMEM((n_z, n_c, rows, chunk), bf16),
            pltpu.VMEM((n_z, n_c, rows, chunk), f32),
            pltpu.VMEM((n_z - 1, n_c, rows, chunk), bf16),
            pltpu.VMEM((n_z + 1, n_c, rows, chunk), bf16),
            pltpu.VMEM((half, depth), f32),
            pltpu.VMEM((depth // 2, wide), bf16),
            pltpu.VMEM((half, wide), bf16),
            dma((3,)),
        ],
        compiler_params=pltpu.CompilerParams(
            collective_id=0, has_side_effects=True, vmem_limit_bytes=56 * 1024 * 1024
        ),
    )(hidden, query_grad, key_grad, value_grad, w_query, w_key, w_value)
    return pl.pallas_call(
        place,
        out_shape=(
            jax.ShapeDtypeStruct((half, depth), bf16),
            jax.ShapeDtypeStruct((rows, q_w), f32),
            jax.ShapeDtypeStruct((rows, k_w), f32),
            jax.ShapeDtypeStruct((rows, k_w), f32),
        ),
        in_specs=[pl.BlockSpec(memory_space=pltpu.VMEM)] * 2,
        out_specs=(pl.BlockSpec(memory_space=pl.ANY),) * 4,
        scratch_shapes=[dma((4,))],
    )(*[pltpu.with_memory_space_constraint(a, pltpu.VMEM) for a in held])


def solution(mesh):
    placed = (
        P(("dp", "tp"), None),
        P("dp", "tp"),
        P("dp", "tp"),
        P("dp", "tp"),
        P(None, "tp"),
        P(None, "tp"),
        P(None, "tp"),
    )
    n_dp, n_tp = mesh.shape["dp"], mesh.shape["tp"]
    body = local
    if n_tp == 2 and n_dp % 4 == 0 and n_dp > 12:
        body = functools.partial(fused, n_dp)
    return jax.shard_map(
        body,
        mesh=mesh,
        in_specs=placed,
        out_specs=(P(("dp", "tp"), None), P("dp", "tp"), P("dp", "tp"), P("dp", "tp")),
        check_vma=False,
    )
```

```python
import functools

import jax
import jax.numpy as jnp
from jax import lax
from jax.experimental import pallas as pl
from jax.experimental.pallas import tpu as pltpu
from jax.sharding import PartitionSpec as P

MESH = pl.DeviceIdType.MESH


def contract_rows(left, right):
    return lax.dot_general(
        left, right, (((0,), (0,)), ((), ())), preferred_element_type=jnp.float32
    )


def contract_cols(left, right):
    return lax.dot_general(
        left, right, (((1,), (1,)), ((), ())), preferred_element_type=jnp.float32
    )


def local(hidden, query_grad, key_grad, value_grad, w_query, w_key, w_value):
    query_width = w_query.shape[1]
    head_width = w_key.shape[1]
    all_grads = jnp.concatenate((query_grad, key_grad, value_grad), axis=1)
    all_weights = jnp.concatenate((w_query, w_key, w_value), axis=1)
    total = contract_rows(lax.all_gather(hidden, "tp", axis=0, tiled=True), all_grads)
    summed = lax.psum_scatter(
        contract_cols(all_grads, all_weights).astype(jnp.bfloat16),
        "tp",
        scatter_dimension=0,
        tiled=True,
    )
    weight_grad = lax.psum_scatter(
        total.astype(jnp.bfloat16), "dp", scatter_dimension=0, tiled=True
    ).astype(jnp.float32)
    grad_query = weight_grad[:, :query_width]
    grad_key = weight_grad[:, query_width : query_width + head_width]
    grad_value = weight_grad[:, query_width + head_width :]
    return (summed, grad_query, grad_key, grad_value)


def targets(n_z, z):
    near_low = z < n_z - 1 - z
    return sorted(
        range(n_z), key=lambda t: (-abs(t - z), t if near_low else -t)
    )


def pick(values, index):
    chosen = jnp.int32(values[0])
    for i, value in enumerate(values[1:]):
        chosen = jnp.where(index == i + 1, jnp.int32(value), chosen)
    return chosen


def kernel(
    n_z, pieces, n_c,
    hidden, query_grad, key_grad, value_grad, w_query, w_key, w_value,
    result, final,
    tokens, grads, weights, head_out, head_in, core_out, core_in,
    total, z_out, z_in, own_head, gathered, own_grads,
    head_sem,
):
    half = hidden.shape[0]
    own_first = hidden.shape[1] // 2
    width = own_first // pieces
    dma = pltpu.SemaphoreType.DMA
    regular = pltpu.SemaphoreType.REGULAR

    def landed(whole, semaphore):
        pltpu.make_async_copy(whole, whole, semaphore).wait()

    def add_heads(j):
        columns = pl.ds(own_first + j * width, width)
        own = own_head[:, columns]
        result[:, columns] = (own + head_in[j].astype(jnp.float32)).astype(result.dtype)

    def scope(
        load_sem, send_sem, x_recv, ytok_recv, ygrad_recv, core_recv, z_recv,
        unit_recv, plane_recv, across_recv, seen_sem, go_sem,
    ):
        dp = lax.axis_index("dp")
        tp = lax.axis_index("tp")
        core = lax.rem(dp, 2)
        y = lax.rem(dp // 2, 2)
        z = dp // 4
        half = hidden.shape[0]
        group = query_grad.shape[0]
        q_w = query_grad.shape[1]
        k_w = key_grad.shape[1]
        rows = final.shape[0]
        pair = 2 * rows
        width = hidden.shape[1] // 2 // pieces
        own_first = hidden.shape[1] // 2
        unit = rows // 2
        chunk = 2 * k_w
        bf16, f32 = jnp.bfloat16, jnp.float32

        x_peer = (dp, 1 - tp)
        core_peer = (dp + 1 - 2 * core, tp)
        y_peer = (dp + 2 - 4 * y, tp)
        at_low, at_high = z == 0, z == n_z - 1
        at_end = jnp.logical_or(at_low, at_high)

        order = [targets(n_z, i) for i in range(n_z)]
        target = [pick([order[i][k] for i in range(n_z)], z) for k in range(n_z)]
        down = [jnp.where(target[k] < z, 1, 0) for k in range(n_z)]

        mine = pl.ds(pl.multiple_of(tp * half, half), half)
        theirs = pl.ds(pl.multiple_of((1 - tp) * half, half), half)
        mine_far = pl.ds(pl.multiple_of(group + tp * half, half), half)

        def columns_of(k, side):
            return pl.ds(pl.multiple_of((target[k] * 2 + side) * pair, pair), pair)

        def load(index, source, place):
            pltpu.make_async_copy(source, place, load_sem.at[index]).start()

        near = pl.ds(0, group)
        far = pl.ds(group, group)

        barrier = pltpu.get_barrier_semaphore()

        def greet(peer):
            pl.semaphore_signal(barrier, inc=1, device_id=peer, device_id_type=MESH)

        greet(x_peer)
        scout = core == 0
        low_peer, high_peer = (dp - 4, tp), (dp + 4, tp)
        around = 3 - jnp.where(at_end, 1, 0)

        def around_line(tell):
            tell(y_peer)
            pl.when(jnp.logical_not(at_low))(lambda: tell(low_peer))
            pl.when(jnp.logical_not(at_high))(lambda: tell(high_peer))

        pl.when(scout)(lambda: around_line(greet))
        pl.when(jnp.logical_not(scout))(lambda: greet(core_peer))
        def start_loads():
            load(0, query_grad, grads.at[near, pl.ds(0, q_w)])
            load(0, key_grad, grads.at[near, pl.ds(q_w, k_w)])
            load(0, value_grad, grads.at[near, pl.ds(q_w + k_w, k_w)])
            load(1, w_query, weights.at[:, pl.ds(0, q_w)])
            load(1, w_key, weights.at[:, pl.ds(q_w, k_w)])
            load(1, w_value, weights.at[:, pl.ds(q_w + k_w, k_w)])
            for k in range(n_z):
                load(2, hidden.at[:, columns_of(k, y)], tokens.at[k, mine, :])

        pl.when(scout)(start_loads)
        pl.semaphore_wait(barrier, 1 + jnp.where(scout, 1 + around, 0))

        def notify(semaphore, peer):
            pl.semaphore_signal(semaphore, inc=1, device_id=peer, device_id_type=MESH)

        def remote(source, place, send, recv, peer):
            return pltpu.make_async_remote_copy(
                src_ref=source, dst_ref=place, send_sem=send, recv_sem=recv,
                device_id=peer, device_id_type=MESH,
            )

        own_copies = [
            remote(
                hidden.at[:, columns_of(k, y)], tokens.at[k, mine, :],
                send_sem.at[0], x_recv.at[k], x_peer,
            )
            for k in range(n_z)
        ]
        fwd_copies = [
            remote(
                tokens.at[k, mine_far, :], tokens.at[k, mine_far, :],
                send_sem.at[0], x_recv.at[k], x_peer,
            )
            for k in range(n_z)
        ]
        ytok_copies = [
            remote(
                hidden.at[:, columns_of(k, 1 - y)], tokens.at[k, mine_far, :],
                send_sem.at[0], ytok_recv.at[k], y_peer,
            )
            for k in range(n_z)
        ]

        def ygrad(source, first, n):
            span = pl.ds(first, source.shape[1])
            return remote(
                source, grads.at[far, span], send_sem.at[1], ygrad_recv.at[n], y_peer
            )

        ygrad_copies = [
            [ygrad(query_grad.at[:, pl.ds(n * chunk, chunk)], n * chunk, n)]
            for n in range(n_c - 1)
        ] + [[ygrad(key_grad, q_w, n_c - 1), ygrad(value_grad, q_w + k_w, n_c - 1)]]
        head_copies = [
            remote(
                head_out.at[j], head_in.at[j], head_sem.at[0],
                head_sem.at[1 if j < pieces - 1 else 2], x_peer,
            )
            for j in range(pieces)
        ]
        core_copies = [
            [
                remote(
                    core_out.at[k, n], core_in.at[k, n],
                    send_sem.at[2], core_recv.at[n if k == 0 else n_c + k - 1], core_peer,
                )
                for n in range(n_c)
            ]
            for k in range(n_z)
        ]
        def place_on(step, below):
            i = below + 1 if order[below][step] > below else below - 1
            if not 0 <= i < n_z or order[below][step] == below:
                return 0
            to = order[below][step]
            if to == i:
                return n_z - 1 if below < i else n_z
            return order[i].index(to)

        z_slot = [pick([place_on(k, i) for i in range(n_z)], z) for k in range(n_z - 1)]
        z_copies = [
            [
                remote(
                    z_out.at[k, n], z_in.at[z_slot[k], n],
                    send_sem.at[3], z_recv.at[z_slot[k], n],
                    (dp + 4 - 8 * down[k], tp),
                )
                for n in range(n_c)
            ]
            for k in range(n_z - 1)
        ]

        def units(source):
            return pl.ds(pl.multiple_of(source * unit, unit), unit)

        fetches = [
            remote(
                source.at[units(dp), :],
                gathered.at[units(dp), pl.ds(first, source.shape[1])],
                send_sem.at[1], plane_recv.at[0], x_peer,
            )
            for source, first in ((w_query, 0), (w_key, q_w), (w_value, q_w + k_w))
        ]
        lend_grads = remote(
            grads.at[theirs, :], own_grads, send_sem.at[1], plane_recv.at[1], x_peer
        )

        def unit_copy(direction, s):
            rows_of = units(dp - 4 * s if direction == 0 else dp + 4 * s)
            return remote(
                gathered.at[rows_of, :], gathered.at[rows_of, :],
                send_sem.at[4], unit_recv.at[z - s if direction == 0 else z + s],
                high_peer if direction == 0 else low_peer,
            )

        def to_sibling(source, across):
            remote(
                gathered.at[units(source), :], gathered.at[units(source), :],
                send_sem.at[1], plane_recv.at[2 + across], core_peer,
            ).start()

        def to_plane(source):
            remote(
                gathered.at[units(source), :], gathered.at[units(source), :],
                send_sem.at[1], across_recv.at[source // 4], y_peer,
            ).start()
            to_sibling(source, 0)

        def loaded(index, whole):
            pltpu.make_async_copy(whole, whole, load_sem.at[index]).wait()

        for copy in own_copies[:1] + fetches:
            copy.start()
        pl.when(jnp.logical_not(scout))(start_loads)

        def start_later_y():
            later = ygrad_copies[0] + ytok_copies[1:2]
            for copies in ygrad_copies[1:]:
                later = later + copies
            for copy in later + ytok_copies[2:]:
                copy.start()

        @pl.when(scout)
        def _():
            ytok_copies[0].start()
            around_line(lambda peer: notify(seen_sem, peer))
            pl.semaphore_wait(seen_sem, around)
            notify(go_sem, core_peer)

        @pl.when(jnp.logical_not(scout))
        def _():
            pl.semaphore_wait(go_sem, 1)
            ytok_copies[0].start()
            start_later_y()

        loaded(0, grads.at[near, :])
        loaded(1, weights)

        def head_piece(j):
            columns = pl.ds(own_first + j * width, width)
            head_out[j] = contract_cols(grads[theirs, :], weights[columns, :]).astype(bf16)
            own_head[:, columns] = contract_cols(grads[mine, :], weights[columns, :])
            columns = pl.ds(j * width, width)
            own_head[:, columns] = contract_cols(grads[mine, :], weights[columns, :])

        def block(k, n, which):
            start = pl.multiple_of(which * rows, rows)
            return contract_rows(
                tokens[k, :, pl.ds(start, rows)], grads[:, pl.ds(n * chunk, chunk)]
            )

        def arrive(k):
            if k == 0:
                loaded(2, tokens.at[:, mine, :])
            landed(tokens.at[k, pl.ds(0, group), :], x_recv.at[k])

        def partial(k, n):
            if k == 0:
                landed(grads.at[far, pl.ds(n * chunk, chunk)], ygrad_recv.at[n])
            core_out[k, n] = block(k, n, 1 - core).astype(bf16)
            core_copies[k][n].start()
            total[k, n] = block(k, n, core)

        def sibling_part(k, n):
            if k == 0:
                landed(core_in.at[k, n], core_recv.at[n])
            elif n == 0:
                landed(core_in.at[k], core_recv.at[n_c + k - 1])
            return core_in[k, n].astype(f32)

        def pass_on(k, n, at_line_end):
            def run():
                summed = total[k, n] + sibling_part(k, n)
                if not at_line_end:
                    landed(z_in.at[k, n], z_recv.at[k, n])
                    summed = summed + z_in[k, n].astype(f32)
                z_out[k, n] = summed.astype(bf16)
                z_copies[k][n].start()

            pl.when(at_end if at_line_end else jnp.logical_not(at_end))(run)

        def finish(n):
            span = pl.ds(n * chunk, chunk)
            final[:, span] = total[last, n] + sibling_part(last, n)

            for slot, edge in ((n_z - 1, at_low), (n_z, at_high)):
                @pl.when(jnp.logical_not(edge))
                def _():
                    landed(z_in.at[slot, n], z_recv.at[slot, n])
                    final[:, span] += z_in[slot, n].astype(f32)

        def add_gathered(i, side):
            start = pl.multiple_of((i * 4 + side * 2) * unit, 2 * unit)
            columns = pl.ds(start, 2 * unit)
            other = contract_cols(own_grads[...], gathered[columns, :])
            result[:, columns] = (own_head[:, columns] + other).astype(result.dtype)

        def relay(s):
            for direction, exists, onward, step in (
                (0, z >= s, jnp.logical_not(at_high), -4),
                (1, z <= n_z - 1 - s, jnp.logical_not(at_low), 4),
            ):
                @pl.when(exists)
                def _():
                    spread(direction, s, onward, dp + step * s)

        def spread(direction, s, onward, source):
            landed(gathered.at[units(source), :], unit_recv.at[z - s if direction == 0 else z + s])
            if s < n_z - 1:
                pl.when(onward)(unit_copy(direction, s).start)
            to_plane(source)

        chunks = range(n_c)
        ready = sent = 0

        def prepare(count):
            nonlocal ready
            for j in range(ready, min(ready + count, pieces)):
                head_piece(j)
            ready = min(ready + count, pieces)

        def send_heads(count):
            nonlocal sent
            for j in range(sent, min(sent + count, ready)):
                head_copies[j].start()
            sent = min(sent + count, ready)

        last = n_z - 1
        in_plane = n_z * unit

        def forward_tokens(k):
            ytok_copies[k].wait_recv()
            fwd_copies[k].start()
            for copy in own_copies[1:3] if k == 0 else own_copies[k + 1 : k + 2]:
                if k != 1:
                    copy.start()
            if k == 1:
                lend_grads.start()
            if k == last:
                send_heads(pieces)

        prepare(1)
        pl.when(scout)(start_later_y)
        prepare(1)
        forward_tokens(0)
        landed(gathered.at[units(dp), :], plane_recv.at[0])
        pl.when(jnp.logical_not(at_high))(unit_copy(0, 0).start)
        pl.when(jnp.logical_not(at_low))(unit_copy(1, 0).start)
        to_plane(dp)
        prepare(2)
        arrive(0)
        partial(0, 0)
        forward_tokens(1)
        pass_on(0, 0, True)
        for n in chunks[1:]:
            if n == n_c - 1:
                relay(1)
            partial(0, n)
            pass_on(0, n, True)
        pass_on(0, 0, False)
        for k in range(1, last):
            forward_tokens(k + 1)
            arrive(k)
            for n in chunks:
                partial(k, n)
            for n in chunks:
                pass_on(k, n, True)
            for n in chunks[1:]:
                pass_on(k - 1, n, False)
            pass_on(k, 0, False)
            if k + 1 < last:
                relay(k + 1)
        for n in chunks[1:]:
            pass_on(last - 1, n, False)
        relay(last)
        arrive(last)
        for n in chunks:
            partial(last, n)
        landed(own_grads, plane_recv.at[1])
        landed(gathered.at[pl.ds(0, in_plane), :], plane_recv.at[2])
        for i in range(n_z):
            add_gathered(i, y)
        for n in chunks[:-1]:
            finish(n)
        for i in reversed(target):
            source = i * 4 + (1 - y) * 2 + core
            landed(gathered.at[units(source), :], across_recv.at[i])
            to_sibling(source, 1)
        finish(n_c - 1)
        landed(gathered.at[pl.ds(0, in_plane), :], plane_recv.at[3])
        for i in range(n_z):
            add_gathered(i, 1 - y)
        units_sent = gathered.at[pl.ds(0, (3 * n_z + 4) * unit), :]
        sources = (tokens.at[:, pl.ds(0, 3 * half), :], units_sent, core_out, z_out)
        for i, source in enumerate(sources):
            landed(source, send_sem.at[i])
        for count, here in ((1, at_end), (n_z + 1, jnp.logical_not(at_end))):
            pl.when(here)(
                lambda: landed(gathered.at[pl.ds(0, count * unit), :], send_sem.at[4])
            )

    pl.run_scoped(
        scope,
        dma((3,)), dma((5,)), dma((n_z,)), dma((n_z,)), dma((n_c,)),
        dma((n_c + n_z - 1,)), dma((n_z + 1, n_c)),
        dma((n_z,)), dma((4,)), dma((n_z,)), regular, regular,
    )
    landed(head_in.at[pl.ds(0, pieces - 1)], head_sem.at[1])
    for j in range(pieces - 1):
        add_heads(j)
    landed(head_in.at[pieces - 1], head_sem.at[2])
    add_heads(pieces - 1)
    landed(head_out, head_sem.at[0])


def place(result, final, out_hidden, out_query, out_key, out_value):
    q_w, k_w = out_query.shape[1], out_key.shape[1]

    def scope(sem):
        pairs = (
            (result, out_hidden),
            (final.at[:, pl.ds(0, q_w)], out_query),
            (final.at[:, pl.ds(q_w, k_w)], out_key),
            (final.at[:, pl.ds(q_w + k_w, k_w)], out_value),
        )
        copies = [
            pltpu.make_async_copy(source, out, sem.at[i])
            for i, (source, out) in enumerate(pairs)
        ]
        for copy in copies:
            copy.start()
        for copy in copies:
            copy.wait()

    pl.run_scoped(scope, pltpu.SemaphoreType.DMA((4,)))


def fused(n_dp, hidden, query_grad, key_grad, value_grad, w_query, w_key, w_value):
    half, depth = hidden.shape
    group = query_grad.shape[0]
    q_w, k_w = w_query.shape[1], w_key.shape[1]
    wide = q_w + 2 * k_w
    rows = depth // n_dp
    if q_w % (2 * k_w) or rows != group or rows % 256 or k_w % 128:
        return local(hidden, query_grad, key_grad, value_grad, w_query, w_key, w_value)
    n_z = n_dp // 4
    n_c = wide // (2 * k_w)
    chunk = 2 * k_w
    pieces = n_z
    width = depth // 2 // pieces
    bf16, f32 = jnp.bfloat16, jnp.float32
    dma = pltpu.SemaphoreType.DMA
    held = pl.pallas_call(
        functools.partial(kernel, n_z, pieces, n_c),
        out_shape=(pltpu.VMEM((half, depth), bf16), pltpu.VMEM((rows, wide), f32)),
        in_specs=[pl.BlockSpec(memory_space=pl.ANY)] * 7,
        out_specs=(pl.BlockSpec(memory_space=pltpu.VMEM),) * 2,
        scratch_shapes=[
            pltpu.VMEM((n_z, 2 * group, 2 * rows), bf16),
            pltpu.VMEM((2 * group, wide), bf16),
            pltpu.VMEM((depth, wide), bf16),
            pltpu.VMEM((pieces, half, width), bf16),
            pltpu.VMEM((pieces, half, width), bf16),
            pltpu.VMEM((n_z, n_c, rows, chunk), bf16),
            pltpu.VMEM((n_z, n_c, rows, chunk), bf16),
            pltpu.VMEM((n_z, n_c, rows, chunk), f32),
            pltpu.VMEM((n_z - 1, n_c, rows, chunk), bf16),
            pltpu.VMEM((n_z + 1, n_c, rows, chunk), bf16),
            pltpu.VMEM((half, depth), f32),
            pltpu.VMEM((depth // 2, wide), bf16),
            pltpu.VMEM((half, wide), bf16),
            dma((3,)),
        ],
        compiler_params=pltpu.CompilerParams(
            collective_id=0, has_side_effects=True, vmem_limit_bytes=56 * 1024 * 1024
        ),
    )(hidden, query_grad, key_grad, value_grad, w_query, w_key, w_value)
    return pl.pallas_call(
        place,
        out_shape=(
            jax.ShapeDtypeStruct((half, depth), bf16),
            jax.ShapeDtypeStruct((rows, q_w), f32),
            jax.ShapeDtypeStruct((rows, k_w), f32),
            jax.ShapeDtypeStruct((rows, k_w), f32),
        ),
        in_specs=[pl.BlockSpec(memory_space=pltpu.VMEM)] * 2,
        out_specs=(pl.BlockSpec(memory_space=pl.ANY),) * 4,
    )(*[pltpu.with_memory_space_constraint(a, pltpu.VMEM) for a in held])


def solution(mesh):
    placed = (
        P(("dp", "tp"), None),
        P("dp", "tp"),
        P("dp", "tp"),
        P("dp", "tp"),
        P(None, "tp"),
        P(None, "tp"),
        P(None, "tp"),
    )
    n_dp, n_tp = mesh.shape["dp"], mesh.shape["tp"]
    body = local
    if n_tp == 2 and n_dp % 4 == 0 and n_dp > 12:
        body = functools.partial(fused, n_dp)
    return jax.shard_map(
        body,
        mesh=mesh,
        in_specs=placed,
        out_specs=(P(("dp", "tp"), None), P("dp", "tp"), P("dp", "tp"), P("dp", "tp")),
        check_vma=False,
    )
```

```python
import functools

import jax
import jax.numpy as jnp
from jax import lax
from jax.experimental import pallas as pl
from jax.experimental.pallas import tpu as pltpu
from jax.sharding import PartitionSpec as P

MESH = pl.DeviceIdType.MESH


def contract_rows(left, right):
    return lax.dot_general(
        left, right, (((0,), (0,)), ((), ())), preferred_element_type=jnp.float32
    )


def contract_cols(left, right):
    return lax.dot_general(
        left, right, (((1,), (1,)), ((), ())), preferred_element_type=jnp.float32
    )


def local(hidden, query_grad, key_grad, value_grad, w_query, w_key, w_value):
    query_width = w_query.shape[1]
    head_width = w_key.shape[1]
    all_grads = jnp.concatenate((query_grad, key_grad, value_grad), axis=1)
    all_weights = jnp.concatenate((w_query, w_key, w_value), axis=1)
    total = contract_rows(lax.all_gather(hidden, "tp", axis=0, tiled=True), all_grads)
    summed = lax.psum_scatter(
        contract_cols(all_grads, all_weights).astype(jnp.bfloat16),
        "tp",
        scatter_dimension=0,
        tiled=True,
    )
    weight_grad = lax.psum_scatter(
        total.astype(jnp.bfloat16), "dp", scatter_dimension=0, tiled=True
    ).astype(jnp.float32)
    grad_query = weight_grad[:, :query_width]
    grad_key = weight_grad[:, query_width : query_width + head_width]
    grad_value = weight_grad[:, query_width + head_width :]
    return (summed, grad_query, grad_key, grad_value)


def targets(n_z, z):
    near_low = z < n_z - 1 - z
    return sorted(
        range(n_z), key=lambda t: (-abs(t - z), t if near_low else -t)
    )


def pick(values, index):
    chosen = jnp.int32(values[0])
    for i, value in enumerate(values[1:]):
        chosen = jnp.where(index == i + 1, jnp.int32(value), chosen)
    return chosen


def kernel(
    n_z, pieces, n_c,
    hidden, query_grad, key_grad, value_grad, w_query, w_key, w_value,
    result, final,
    tokens, grads, weights, head_out, head_in, core_out, core_in,
    total, z_out, z_in, own_head, gathered, own_grads,
):
    half = hidden.shape[0]
    own_first = hidden.shape[1] // 2
    width = own_first // pieces
    dma = pltpu.SemaphoreType.DMA
    regular = pltpu.SemaphoreType.REGULAR

    def landed(whole, semaphore):
        pltpu.make_async_copy(whole, whole, semaphore).wait()

    def add_heads(j):
        columns = pl.ds(own_first + j * width, width)
        own = own_head[:, columns]
        result[:, columns] = (own + head_in[j].astype(jnp.float32)).astype(result.dtype)

    def scope(
        load_sem, send_sem, x_recv, ytok_recv, ygrad_recv, core_recv, z_recv,
        unit_recv, plane_recv, across_recv, seen_sem, go_sem,
        head_sem,
    ):
        dp = lax.axis_index("dp")
        tp = lax.axis_index("tp")
        core = lax.rem(dp, 2)
        y = lax.rem(dp // 2, 2)
        z = dp // 4
        half = hidden.shape[0]
        group = query_grad.shape[0]
        q_w = query_grad.shape[1]
        k_w = key_grad.shape[1]
        rows = final.shape[0]
        pair = 2 * rows
        width = hidden.shape[1] // 2 // pieces
        own_first = hidden.shape[1] // 2
        unit = rows // 2
        chunk = 2 * k_w
        bf16, f32 = jnp.bfloat16, jnp.float32

        x_peer = (dp, 1 - tp)
        core_peer = (dp + 1 - 2 * core, tp)
        y_peer = (dp + 2 - 4 * y, tp)
        at_low, at_high = z == 0, z == n_z - 1
        at_end = jnp.logical_or(at_low, at_high)

        order = [targets(n_z, i) for i in range(n_z)]
        target = [pick([order[i][k] for i in range(n_z)], z) for k in range(n_z)]
        down = [jnp.where(target[k] < z, 1, 0) for k in range(n_z)]

        mine = pl.ds(pl.multiple_of(tp * half, half), half)
        theirs = pl.ds(pl.multiple_of((1 - tp) * half, half), half)
        mine_far = pl.ds(pl.multiple_of(group + tp * half, half), half)

        def columns_of(k, side):
            return pl.ds(pl.multiple_of((target[k] * 2 + side) * pair, pair), pair)

        def load(index, source, place):
            pltpu.make_async_copy(source, place, load_sem.at[index]).start()

        near = pl.ds(0, group)
        far = pl.ds(group, group)

        barrier = pltpu.get_barrier_semaphore()

        def greet(peer):
            pl.semaphore_signal(barrier, inc=1, device_id=peer, device_id_type=MESH)

        greet(x_peer)
        scout = core == 0
        low_peer, high_peer = (dp - 4, tp), (dp + 4, tp)
        around = 3 - jnp.where(at_end, 1, 0)

        def around_line(tell):
            tell(y_peer)
            pl.when(jnp.logical_not(at_low))(lambda: tell(low_peer))
            pl.when(jnp.logical_not(at_high))(lambda: tell(high_peer))

        pl.when(scout)(lambda: around_line(greet))
        pl.when(jnp.logical_not(scout))(lambda: greet(core_peer))
        def start_loads():
            load(0, query_grad, grads.at[near, pl.ds(0, q_w)])
            load(0, key_grad, grads.at[near, pl.ds(q_w, k_w)])
            load(0, value_grad, grads.at[near, pl.ds(q_w + k_w, k_w)])
            load(1, w_query, weights.at[:, pl.ds(0, q_w)])
            load(1, w_key, weights.at[:, pl.ds(q_w, k_w)])
            load(1, w_value, weights.at[:, pl.ds(q_w + k_w, k_w)])
            for k in range(n_z):
                load(2, hidden.at[:, columns_of(k, y)], tokens.at[k, mine, :])

        pl.when(scout)(start_loads)
        pl.semaphore_wait(barrier, 1 + jnp.where(scout, 1 + around, 0))

        def notify(semaphore, peer):
            pl.semaphore_signal(semaphore, inc=1, device_id=peer, device_id_type=MESH)

        def remote(source, place, send, recv, peer):
            return pltpu.make_async_remote_copy(
                src_ref=source, dst_ref=place, send_sem=send, recv_sem=recv,
                device_id=peer, device_id_type=MESH,
            )

        own_copies = [
            remote(
                hidden.at[:, columns_of(k, y)], tokens.at[k, mine, :],
                send_sem.at[0], x_recv.at[k], x_peer,
            )
            for k in range(n_z)
        ]
        fwd_copies = [
            remote(
                tokens.at[k, mine_far, :], tokens.at[k, mine_far, :],
                send_sem.at[0], x_recv.at[k], x_peer,
            )
            for k in range(n_z)
        ]
        ytok_copies = [
            remote(
                hidden.at[:, columns_of(k, 1 - y)], tokens.at[k, mine_far, :],
                send_sem.at[0], ytok_recv.at[k], y_peer,
            )
            for k in range(n_z)
        ]

        def ygrad(source, first, n):
            span = pl.ds(first, source.shape[1])
            return remote(
                source, grads.at[far, span], send_sem.at[1], ygrad_recv.at[n], y_peer
            )

        ygrad_copies = [
            [ygrad(query_grad.at[:, pl.ds(n * chunk, chunk)], n * chunk, n)]
            for n in range(n_c - 1)
        ] + [[ygrad(key_grad, q_w, n_c - 1), ygrad(value_grad, q_w + k_w, n_c - 1)]]
        head_copies = [
            remote(
                head_out.at[j], head_in.at[j], head_sem.at[0],
                head_sem.at[1 if j < pieces - 1 else 2], x_peer,
            )
            for j in range(pieces)
        ]
        core_copies = [
            [
                remote(
                    core_out.at[k, n], core_in.at[k, n],
                    send_sem.at[2], core_recv.at[n if k == 0 else n_c + k - 1], core_peer,
                )
                for n in range(n_c)
            ]
            for k in range(n_z)
        ]
        def place_on(step, below):
            i = below + 1 if order[below][step] > below else below - 1
            if not 0 <= i < n_z or order[below][step] == below:
                return 0
            to = order[below][step]
            if to == i:
                return n_z - 1 if below < i else n_z
            return order[i].index(to)

        z_slot = [pick([place_on(k, i) for i in range(n_z)], z) for k in range(n_z - 1)]
        z_copies = [
            [
                remote(
                    z_out.at[k, n], z_in.at[z_slot[k], n],
                    send_sem.at[3], z_recv.at[z_slot[k], n],
                    (dp + 4 - 8 * down[k], tp),
                )
                for n in range(n_c)
            ]
            for k in range(n_z - 1)
        ]

        def units(source):
            return pl.ds(pl.multiple_of(source * unit, unit), unit)

        fetches = [
            remote(
                source.at[units(dp), :],
                gathered.at[units(dp), pl.ds(first, source.shape[1])],
                send_sem.at[1], plane_recv.at[0], x_peer,
            )
            for source, first in ((w_query, 0), (w_key, q_w), (w_value, q_w + k_w))
        ]
        lend_grads = remote(
            grads.at[theirs, :], own_grads, send_sem.at[1], plane_recv.at[1], x_peer
        )

        def unit_copy(direction, s):
            rows_of = units(dp - 4 * s if direction == 0 else dp + 4 * s)
            return remote(
                gathered.at[rows_of, :], gathered.at[rows_of, :],
                send_sem.at[4], unit_recv.at[z - s if direction == 0 else z + s],
                high_peer if direction == 0 else low_peer,
            )

        def to_sibling(source, across):
            remote(
                gathered.at[units(source), :], gathered.at[units(source), :],
                send_sem.at[1], plane_recv.at[2 + across], core_peer,
            ).start()

        def to_plane(source):
            remote(
                gathered.at[units(source), :], gathered.at[units(source), :],
                send_sem.at[1], across_recv.at[source // 4], y_peer,
            ).start()
            to_sibling(source, 0)

        def loaded(index, whole):
            pltpu.make_async_copy(whole, whole, load_sem.at[index]).wait()

        for copy in own_copies[:1] + fetches:
            copy.start()
        pl.when(jnp.logical_not(scout))(start_loads)

        def start_later_y():
            later = ygrad_copies[0] + ytok_copies[1:2]
            for copies in ygrad_copies[1:]:
                later = later + copies
            for copy in later + ytok_copies[2:]:
                copy.start()

        @pl.when(scout)
        def _():
            ytok_copies[0].start()
            around_line(lambda peer: notify(seen_sem, peer))
            pl.semaphore_wait(seen_sem, around)
            notify(go_sem, core_peer)

        @pl.when(jnp.logical_not(scout))
        def _():
            pl.semaphore_wait(go_sem, 1)
            ytok_copies[0].start()
            start_later_y()

        loaded(0, grads.at[near, :])
        loaded(1, weights)

        def head_piece(j):
            columns = pl.ds(own_first + j * width, width)
            head_out[j] = contract_cols(grads[theirs, :], weights[columns, :]).astype(bf16)
            own_head[:, columns] = contract_cols(grads[mine, :], weights[columns, :])
            columns = pl.ds(j * width, width)
            own_head[:, columns] = contract_cols(grads[mine, :], weights[columns, :])

        def block(k, n, which):
            start = pl.multiple_of(which * rows, rows)
            return contract_rows(
                tokens[k, :, pl.ds(start, rows)], grads[:, pl.ds(n * chunk, chunk)]
            )

        def arrive(k):
            if k == 0:
                loaded(2, tokens.at[:, mine, :])
            landed(tokens.at[k, pl.ds(0, group), :], x_recv.at[k])

        def partial(k, n):
            if k == 0:
                landed(grads.at[far, pl.ds(n * chunk, chunk)], ygrad_recv.at[n])
            core_out[k, n] = block(k, n, 1 - core).astype(bf16)
            core_copies[k][n].start()
            total[k, n] = block(k, n, core)

        def sibling_part(k, n):
            if k == 0:
                landed(core_in.at[k, n], core_recv.at[n])
            elif n == 0:
                landed(core_in.at[k], core_recv.at[n_c + k - 1])
            return core_in[k, n].astype(f32)

        def pass_on(k, n, at_line_end):
            def run():
                summed = total[k, n] + sibling_part(k, n)
                if not at_line_end:
                    landed(z_in.at[k, n], z_recv.at[k, n])
                    summed = summed + z_in[k, n].astype(f32)
                z_out[k, n] = summed.astype(bf16)
                z_copies[k][n].start()

            pl.when(at_end if at_line_end else jnp.logical_not(at_end))(run)

        def finish(n):
            span = pl.ds(n * chunk, chunk)
            final[:, span] = total[last, n] + sibling_part(last, n)

            for slot, edge in ((n_z - 1, at_low), (n_z, at_high)):
                @pl.when(jnp.logical_not(edge))
                def _():
                    landed(z_in.at[slot, n], z_recv.at[slot, n])
                    final[:, span] += z_in[slot, n].astype(f32)

        def add_gathered(i, side):
            start = pl.multiple_of((i * 4 + side * 2) * unit, 2 * unit)
            columns = pl.ds(start, 2 * unit)
            other = contract_cols(own_grads[...], gathered[columns, :])
            result[:, columns] = (own_head[:, columns] + other).astype(result.dtype)

        def relay(s):
            for direction, exists, onward, step in (
                (0, z >= s, jnp.logical_not(at_high), -4),
                (1, z <= n_z - 1 - s, jnp.logical_not(at_low), 4),
            ):
                @pl.when(exists)
                def _():
                    spread(direction, s, onward, dp + step * s)

        def spread(direction, s, onward, source):
            landed(gathered.at[units(source), :], unit_recv.at[z - s if direction == 0 else z + s])
            if s < n_z - 1:
                pl.when(onward)(unit_copy(direction, s).start)
            to_plane(source)

        chunks = range(n_c)
        ready = sent = 0

        def prepare(count):
            nonlocal ready
            for j in range(ready, min(ready + count, pieces)):
                head_piece(j)
            ready = min(ready + count, pieces)

        def send_heads(count):
            nonlocal sent
            for j in range(sent, min(sent + count, ready)):
                head_copies[j].start()
            sent = min(sent + count, ready)

        last = n_z - 1
        in_plane = n_z * unit

        def forward_tokens(k):
            ytok_copies[k].wait_recv()
            fwd_copies[k].start()
            for copy in own_copies[1:3] if k == 0 else own_copies[k + 1 : k + 2]:
                if k != 1:
                    copy.start()
            if k == 1:
                lend_grads.start()
            if k == last:
                send_heads(pieces)

        prepare(1)
        pl.when(scout)(start_later_y)
        prepare(1)
        forward_tokens(0)
        landed(gathered.at[units(dp), :], plane_recv.at[0])
        pl.when(jnp.logical_not(at_high))(unit_copy(0, 0).start)
        pl.when(jnp.logical_not(at_low))(unit_copy(1, 0).start)
        to_plane(dp)
        prepare(2)
        arrive(0)
        partial(0, 0)
        forward_tokens(1)
        pass_on(0, 0, True)
        for n in chunks[1:]:
            if n == n_c - 1:
                relay(1)
            partial(0, n)
            pass_on(0, n, True)
        pass_on(0, 0, False)
        for k in range(1, last):
            forward_tokens(k + 1)
            arrive(k)
            for n in chunks:
                partial(k, n)
            for n in chunks:
                pass_on(k, n, True)
            for n in chunks[1:]:
                pass_on(k - 1, n, False)
            pass_on(k, 0, False)
            if k + 1 < last:
                relay(k + 1)
        for n in chunks[1:]:
            pass_on(last - 1, n, False)
        relay(last)
        arrive(last)
        for n in chunks:
            partial(last, n)
        landed(own_grads, plane_recv.at[1])
        landed(gathered.at[pl.ds(0, in_plane), :], plane_recv.at[2])
        for i in range(n_z):
            add_gathered(i, y)
        for n in chunks[:-1]:
            finish(n)
        for i in reversed(target):
            source = i * 4 + (1 - y) * 2 + core
            landed(gathered.at[units(source), :], across_recv.at[i])
            to_sibling(source, 1)
        finish(n_c - 1)
        landed(gathered.at[pl.ds(0, in_plane), :], plane_recv.at[3])
        for i in range(n_z):
            add_gathered(i, 1 - y)
        units_sent = gathered.at[pl.ds(0, (3 * n_z + 4) * unit), :]
        sources = (tokens.at[:, pl.ds(0, 3 * half), :], units_sent, core_out, z_out)
        for i, source in enumerate(sources):
            landed(source, send_sem.at[i])
        for count, here in ((1, at_end), (n_z + 1, jnp.logical_not(at_end))):
            pl.when(here)(
                lambda: landed(gathered.at[pl.ds(0, count * unit), :], send_sem.at[4])
            )
        landed(head_in.at[pl.ds(0, pieces - 1)], head_sem.at[1])
        for j in range(pieces - 1):
            add_heads(j)
        landed(head_in.at[pieces - 1], head_sem.at[2])
        add_heads(pieces - 1)
        landed(head_out, head_sem.at[0])

    pl.run_scoped(
        scope,
        dma((3,)), dma((5,)), dma((n_z,)), dma((n_z,)), dma((n_c,)),
        dma((n_c + n_z - 1,)), dma((n_z + 1, n_c)),
        dma((n_z,)), dma((4,)), dma((n_z,)), regular, regular, dma((3,)),
    )


def place(result, final, out_hidden, out_query, out_key, out_value):
    q_w, k_w = out_query.shape[1], out_key.shape[1]

    def scope(sem):
        pairs = (
            (result, out_hidden),
            (final.at[:, pl.ds(0, q_w)], out_query),
            (final.at[:, pl.ds(q_w, k_w)], out_key),
            (final.at[:, pl.ds(q_w + k_w, k_w)], out_value),
        )
        copies = [
            pltpu.make_async_copy(source, out, sem.at[i])
            for i, (source, out) in enumerate(pairs)
        ]
        for copy in copies:
            copy.start()
        for copy in copies:
            copy.wait()

    pl.run_scoped(scope, pltpu.SemaphoreType.DMA((4,)))


def fused(n_dp, hidden, query_grad, key_grad, value_grad, w_query, w_key, w_value):
    half, depth = hidden.shape
    group = query_grad.shape[0]
    q_w, k_w = w_query.shape[1], w_key.shape[1]
    wide = q_w + 2 * k_w
    rows = depth // n_dp
    if q_w % (2 * k_w) or rows != group or rows % 256 or k_w % 128:
        return local(hidden, query_grad, key_grad, value_grad, w_query, w_key, w_value)
    n_z = n_dp // 4
    n_c = wide // (2 * k_w)
    chunk = 2 * k_w
    pieces = n_z
    width = depth // 2 // pieces
    bf16, f32 = jnp.bfloat16, jnp.float32
    dma = pltpu.SemaphoreType.DMA
    held = pl.pallas_call(
        functools.partial(kernel, n_z, pieces, n_c),
        out_shape=(pltpu.VMEM((half, depth), bf16), pltpu.VMEM((rows, wide), f32)),
        in_specs=[pl.BlockSpec(memory_space=pl.ANY)] * 7,
        out_specs=(pl.BlockSpec(memory_space=pltpu.VMEM),) * 2,
        scratch_shapes=[
            pltpu.VMEM((n_z, 2 * group, 2 * rows), bf16),
            pltpu.VMEM((2 * group, wide), bf16),
            pltpu.VMEM((depth, wide), bf16),
            pltpu.VMEM((pieces, half, width), bf16),
            pltpu.VMEM((pieces, half, width), bf16),
            pltpu.VMEM((n_z, n_c, rows, chunk), bf16),
            pltpu.VMEM((n_z, n_c, rows, chunk), bf16),
            pltpu.VMEM((n_z, n_c, rows, chunk), f32),
            pltpu.VMEM((n_z - 1, n_c, rows, chunk), bf16),
            pltpu.VMEM((n_z + 1, n_c, rows, chunk), bf16),
            pltpu.VMEM((half, depth), f32),
            pltpu.VMEM((depth // 2, wide), bf16),
            pltpu.VMEM((half, wide), bf16),
        ],
        compiler_params=pltpu.CompilerParams(
            collective_id=0, has_side_effects=True, vmem_limit_bytes=56 * 1024 * 1024
        ),
    )(hidden, query_grad, key_grad, value_grad, w_query, w_key, w_value)
    return pl.pallas_call(
        place,
        out_shape=(
            jax.ShapeDtypeStruct((half, depth), bf16),
            jax.ShapeDtypeStruct((rows, q_w), f32),
            jax.ShapeDtypeStruct((rows, k_w), f32),
            jax.ShapeDtypeStruct((rows, k_w), f32),
        ),
        in_specs=[pl.BlockSpec(memory_space=pltpu.VMEM)] * 2,
        out_specs=(pl.BlockSpec(memory_space=pl.ANY),) * 4,
    )(*[pltpu.with_memory_space_constraint(a, pltpu.VMEM) for a in held])


def solution(mesh):
    placed = (
        P(("dp", "tp"), None),
        P("dp", "tp"),
        P("dp", "tp"),
        P("dp", "tp"),
        P(None, "tp"),
        P(None, "tp"),
        P(None, "tp"),
    )
    n_dp, n_tp = mesh.shape["dp"], mesh.shape["tp"]
    body = local
    if n_tp == 2 and n_dp % 4 == 0 and n_dp > 12:
        body = functools.partial(fused, n_dp)
    return jax.shard_map(
        body,
        mesh=mesh,
        in_specs=placed,
        out_specs=(P(("dp", "tp"), None), P("dp", "tp"), P("dp", "tp"), P("dp", "tp")),
        check_vma=False,
    )
```
